32 devices in a mesh: rows: 4 (over z), cx: 2 (over y), cy: 4 (over x, core).
Axes of the slice: x: 2, y: 2, z: 4, core: 2. Of those that a mesh axis runs over, the one named last changes fastest.
Arguments:
- rows_data: float32 [2048, 1024], P(('rows', 'cx', 'cy')), may hold values from -6 to 6
- owner_rows: int32 [2048, 1], P(('rows', 'cx', 'cy')), may hold values from 0 to 7; in each aligned block of 64 rows (0 to 63, 64 to 127, ...) at most 16 rows name the same one
- slot_rows: int32 [2048], P(('rows', 'cx', 'cy')), may hold values from 0 to 2047
- centroids: float32 [16384, 1024], P(('cx', 'cy'), 'rows'), may hold values from -6 to 6
- counts: float32 [16384], P(('cx', 'cy')), may hold values from 1 to 100
- owner_cent: int32 [16384, 1], P(('cx', 'cy')), may hold values from 0 to 7; in each aligned block of 2048 rows (0 to 2047, 2048 to 4095, ...) at most 512 rows name the same one
- slot_cent: int32 [16384], P(('cx', 'cy')), may hold values from 0 to 511
- upper: float32 [4096, 1024], P(('cx', 'cy'), 'rows'), may hold values from -6 to 6
- upper_counts: float32 [4096], P(('cx', 'cy')), may hold values from 1 to 100
Outputs:
- moved: float32 [16384, 1024], P(('cx', 'cy'), 'rows')
- new_counts: float32 [16384], P(('cx', 'cy'))
- new_upper: float32 [4096, 1024], P(('cx', 'cy'), 'rows')
- new_upper_counts: float32 [4096], P(('cx', 'cy'))
The draws below stay inside these ranges and needn't reach their ends.
Inputs may be any that keep to these rules, and one draw needn't show every extreme that they name: `owner_rows`: the rows of one device name each value at most 16 times, and some device reaches it. `owner_cent`: the 2048 level-1 centroids of one shard name each value at most 512 times, and some shard reaches it.
All inputs are finite; a program needn't handle non-finite values.
Results may differ from the reference program's by a relative error of at most 0.00002.
Values sent between devices are 32-bit elements; how exact they have to be, the bound alone decides.
A program may use at most 64 MiB of HBM per device.

```python
import math
import jax
import jax.numpy as jnp
import numpy as np

D = 1024
C1_DEV = 2048
K2 = 4096
TOK_DEV = 64
SHARDS = 8
C1 = 16384
K2_DEV = 512
ROWS_ALL = 2048
CAP1 = 16
CAP2 = 512


def plant(entries, rng, smallest, top_value):
    spot = [jax.random.randint(jax.random.fold_in(rng, axis), (), 0, length) for axis, length in enumerate(entries.shape)]
    main_axis = entries.shape.index(max(entries.shape))
    beside = spot[:main_axis] + [(spot[main_axis] + 1) % entries.shape[main_axis]] + spot[main_axis + 1:]
    return entries.at[tuple(spot)].set(smallest).at[tuple(beside)].set(top_value)


def block_levels(key, extent, split, least, high):
    gain, own = 1.0, jax.random.fold_in(key, 6)
    for dim, blocks in split:
        heights = jnp.exp(jax.random.uniform(jax.random.fold_in(own, dim), (blocks,), jnp.float32, least / len(split), high / len(split)))
        gain = gain * jnp.repeat(heights, extent[dim] // blocks).reshape([-1 if axis == dim else 1 for axis in range(len(extent))])
    return gain


def shared_out(key, own, number, rows, amount, top, limit, slope):
    ranking = jax.random.permutation(key, amount)
    heavy_load, ordinary = shares(amount, rows * top, limit, slope, True), shares(amount, rows * top, limit, slope, False)
    places = jnp.arange(amount)

    def named(lengths, offset_by):
        used = int((lengths > 0).sum())
        fixed = max(1, used // 4)
        passed = fixed + (places - fixed + offset_by * (used - fixed)) % max(1, amount - fixed)
        return jnp.zeros((amount,), jnp.int32).at[ranking[jnp.where(places < fixed, places, passed)]].set(jnp.asarray(lengths, jnp.int32))

    lengths = jnp.where(number % 4 == 0, named(heavy_load, number // 4), named(ordinary, number - number // 4 - 1))
    mixed = jax.random.permutation(jax.random.fold_in(own, 3), amount)
    giver, receiver = mixed[0:amount // 2 * 2:2], mixed[1:amount // 2 * 2:2]
    room = jnp.minimum(lengths[giver] - 1, limit - lengths[receiver]) // 2
    room = jnp.where((giver == ranking[0]) | (receiver == ranking[0]) | (lengths[receiver] == 0), 0, jnp.maximum(room, 0))
    passed = jax.random.randint(jax.random.fold_in(own, 4), (amount // 2,), 0, 1 << 20) % (room + 1)
    lengths = lengths.at[giver].add(-passed).at[receiver].add(passed)
    members = jnp.searchsorted(jnp.cumsum(lengths), jnp.arange(rows * top), side="right").astype(jnp.int32)
    listing = members.reshape(top, rows).T
    listing = listing[jax.random.permutation(jax.random.fold_in(own, 1), rows)]
    offset_by = jax.random.randint(jax.random.fold_in(own, 2), (rows, 1), 0, top)
    return jnp.take_along_axis(listing, (jnp.arange(top)[None, :] + offset_by) % top, axis=1)


def shares(count, total, bound, slope, full):
    weights = [(1 << 20) // math.isqrt(standing ** slope) + 1 for standing in range(1, count + 1)]
    largest = bound if full else min(bound, max(-(-total // count), total * weights[0] // sum(weights)))
    least = 1 if total - largest >= count - 1 else 0
    given, rest = [largest] + [least] * (count - 1), total - largest - least * (count - 1)
    while rest > 0:
        free = [i for i in range(1, count) if given[i] < largest] or [i for i in range(1, count) if given[i] < bound]
        mass, left = sum([weights[i] for i in free]), rest
        for i in free:
            extra = min(bound - given[i], max(1, left * weights[i] // mass), rest)
            given[i] = given[i] + extra
            rest = rest - extra
    return np.array(given)


def centred(stream_key, dims, deviation, reach, pieces=(), dtype=jnp.bfloat16):
    entries = jax.random.normal(stream_key, dims, jnp.float32) * deviation
    if len(pieces) > 0:
        entries = block_levels(stream_key, dims, pieces, -0.22, 0.18) * entries
    return jnp.clip(entries, min=-reach, max=reach).astype(dtype)


def setup_inputs(seed: int = 0) -> dict:
    arg_keys = jax.random.split(jax.random.key(seed), 10)
    rows_data = centred(arg_keys[0], (ROWS_ALL, D), 1.0, 6.0, ((0, 32),), jnp.float32)
    owner_rows_keys = jax.random.split(jax.random.fold_in(arg_keys[1], 1), ROWS_ALL // TOK_DEV)
    owner_rows_turns = jax.random.permutation(jax.random.fold_in(arg_keys[1], 3), ROWS_ALL // TOK_DEV)
    owner_rows = jax.vmap(lambda own, number: shared_out(jax.random.fold_in(arg_keys[1], 2), own, number, TOK_DEV, SHARDS, 1, CAP1, 2))(owner_rows_keys, owner_rows_turns).reshape((ROWS_ALL, 1))
    slot_rows = plant(jax.random.randint(arg_keys[2], (ROWS_ALL,), 0, C1_DEV), jax.random.fold_in(arg_keys[2], 1), 0, C1_DEV - 1).astype(jnp.int32)
    centroids = centred(arg_keys[3], (C1, D), 1.0, 6.0, ((0, 8), (1, 4)), jnp.float32)
    counts = jnp.clip(jnp.exp(math.log(100.0) - 4.6051702 * jax.random.uniform(arg_keys[4], (C1,), jnp.float32) ** block_levels(arg_keys[4], (C1,), ((0, 8),), -0.2, 0.2)), 1.0, 100.0)
    owner_cent_keys = jax.random.split(jax.random.fold_in(arg_keys[5], 1), C1 // C1_DEV)
    owner_cent_turns = jax.random.permutation(jax.random.fold_in(arg_keys[5], 3), C1 // C1_DEV)
    owner_cent = jax.vmap(lambda own, number: shared_out(jax.random.fold_in(arg_keys[5], 2), own, number, C1_DEV, SHARDS, 1, CAP2, 2))(owner_cent_keys, owner_cent_turns).reshape((C1, 1))
    slot_cent = plant(jax.random.randint(arg_keys[6], (C1,), 0, K2_DEV), jax.random.fold_in(arg_keys[6], 1), 0, K2_DEV - 1).astype(jnp.int32)
    upper = centred(arg_keys[7], (K2, D), 1.0, 6.0, ((0, 8), (1, 4)), jnp.float32)
    upper_counts = jnp.clip(jnp.exp(math.log(100.0) - 4.6051702 * jax.random.uniform(arg_keys[8], (K2,), jnp.float32) ** block_levels(arg_keys[8], (K2,), ((0, 8),), -0.2, 0.2)), 1.0, 100.0)
    return dict(rows_data=rows_data, owner_rows=owner_rows, slot_rows=slot_rows, centroids=centroids, counts=counts, owner_cent=owner_cent, slot_cent=slot_cent, upper=upper, upper_counts=upper_counts)


def reference(rows_data, owner_rows, slot_rows, centroids, counts, owner_cent, slot_cent, upper, upper_counts):
    lower_ids = owner_rows[:, 0] * C1_DEV + slot_rows
    summed = jax.ops.segment_sum(rows_data, lower_ids, num_segments=C1)
    member_counts = jax.ops.segment_sum(jnp.ones(lower_ids.shape, jnp.float32), lower_ids, num_segments=C1)
    new_counts = counts + member_counts
    moved = centroids + (summed - member_counts[:, None] * centroids) / new_counts[:, None]
    upper_ids = owner_cent[:, 0] * K2_DEV + slot_cent
    upper_summed = jax.ops.segment_sum(moved, upper_ids, num_segments=K2)
    upper_members = jax.ops.segment_sum(jnp.ones(upper_ids.shape, jnp.float32), upper_ids, num_segments=K2)
    new_upper_counts = upper_counts + upper_members
    new_upper = upper + (upper_summed - upper_members[:, None] * upper) / new_upper_counts[:, None]
    return moved, new_counts, new_upper, new_upper_counts
```

```python
import functools
import types

import jax
import jax.numpy as jnp
from jax import lax
from jax.experimental import pallas as pl
from jax.experimental.pallas import tpu as pltpu
from jax.sharding import PartitionSpec as P

MESH = pl.DeviceIdType.MESH
LANES = 128
CORES = 2
SPAN = 256
bf16, f32, i32 = jnp.bfloat16, jnp.float32, jnp.int32


def pieces(x):
    first = x.astype(bf16)
    return first, (x - first.astype(f32)).astype(bf16)


def halves(x):
    return x[:, :LANES] + x[:, LANES : 2 * LANES]


def square(size):
    up = lax.broadcasted_iota(i32, (size, size), 0)
    return up == lax.broadcasted_iota(i32, (size, size), 1)


def to_column(row, same):
    size = row.shape[1]
    return jnp.sum(jnp.where(same, jnp.broadcast_to(row, (size, size)), 0.0), axis=1, keepdims=True)


def to_row(column, same):
    return jnp.sum(jnp.where(same, jnp.broadcast_to(column, same.shape), 0.0), axis=0, keepdims=True)


def each(count, step):
    if count == 1:
        step(0)
    elif count > 1:
        lax.fori_loop(0, count, lambda e, c: (step(e), c)[1], 0)


def one_hot(row_of, lines, out, height):
    span = min(SPAN, height)
    spots = lax.broadcasted_iota(i32, (span, LANES), 0).astype(f32).astype(bf16)
    one, zero = jnp.ones((span, LANES), bf16), jnp.zeros((span, LANES), bf16)
    for q in range(height // span):
        for b in range(lines):
            row = jnp.broadcast_to(row_of(b) - float(q * span), (16, LANES)).astype(bf16)
            row = jnp.concatenate([row] * (span // 16), axis=0)
            out[q * span : (q + 1) * span, b * LANES : (b + 1) * LANES] = jnp.where(row == spots, one, zero)


def fused_kernel(
    names, sizes, rows_h, owner_h, slot_h, cent_h, counts_h, oc_h, sc_h, upper_h, weights_h,
    moved, news, newup, upnews, *scratch,
):
    s = types.SimpleNamespace(**dict(zip(names, scratch)))
    zs, ys, xs, capacity, height = sizes
    chips, cys = ys * xs, xs * CORES
    shards = chips * CORES
    batch = rows_h.shape[0]
    count, width = cent_h.shape
    parts = width // LANES
    lines = count // LANES
    slots = upper_h.shape[0]
    half = slots // 2
    tall, block = weights_h.shape
    spots = shards * capacity
    per = LANES // capacity
    across = zs * spots // LANES
    joined = across * LANES

    z, y, cy = lax.axis_index("rows"), lax.axis_index("cx"), lax.axis_index("cy")
    x, core = lax.div(cy, CORES), lax.rem(cy, CORES)
    me = y * cys + cy
    other = {"cx": y, "cy": x * CORES + 1 - core}

    def mate(d):
        if zs & (zs - 1):
            return lax.rem(z + d, zs)
        at = z
        bit = 1
        while bit <= d:
            if d & bit:
                at = at + bit * (1 - 2 * lax.rem(lax.div(z, bit), 2))
            bit *= 2
        return at

    mates = {d: {"rows": mate(d)} for d in range(1, zs)}
    peers = {}
    for p in range(1, shards):
        t = lax.rem(me + p, shards)
        peers[p] = {"cx": lax.div(t, cys), "cy": lax.rem(t, cys)}

    barrier = pltpu.get_barrier_semaphore()
    for peer in list(mates.values()) + list(peers.values()):
        pl.semaphore_signal(barrier, inc=1, device_id=peer, device_id_type=MESH)

    loads = [
        pltpu.make_async_copy(src, dst, s.ld.at[i])
        for i, (src, dst) in enumerate([
            (oc_h, s.oc), (sc_h, s.sc), (cent_h, s.cent), (owner_h, s.owner), (slot_h, s.slot),
            (rows_h, s.rows), (counts_h, s.counts), (upper_h, s.upper), (weights_h, s.weights),
        ])
    ]
    for copy in loads:
        copy.start()

    def remote(src, dst, send, recv, peer):
        return pltpu.make_async_remote_copy(
            src_ref=src, dst_ref=dst, send_sem=send, recv_sem=recv, device_id=peer, device_id_type=MESH
        )

    def started(*args):
        copy = remote(*args)
        copy.start()
        return copy

    same = square(LANES)
    lane = lax.broadcasted_iota(i32, (LANES, LANES), 1)

    regions = {
        "diag": ((ys - 1) * (xs - 1), lambda e: (1 + lax.div(e, xs - 1), 1 + lax.rem(e, xs - 1))),
        "dy": (ys - 1, lambda e: (1 + e, 0)),
        "dx": (xs - 1, lambda e: (0, 1 + e)),
        "own": (1, lambda e: (0, 0)),
    }

    def region(name, step):
        number, where = regions[name]

        def run(e):
            if isinstance(e, int):
                e = jnp.int32(e)
            step(*where(e))

        each(number, run)

    def shard_at(dy, dx, side):
        return (lax.rem(y + dy, ys) * xs + lax.rem(x + dx, xs)) * CORES + side

    loads[0].wait()
    loads[1].wait()
    for b in range(lines):
        s.own[b : b + 1, :] = s.oc[0:1, b * LANES : (b + 1) * LANES]
    s.uid[...] = (s.own[...] * slots + s.sc[...]).astype(f32)
    loads[2].wait()

    def split(b, c):
        here = pl.ds(pl.multiple_of(b * SPAN, SPAN), SPAN)
        for h in range(parts):
            hi, lo = pieces(s.cent[here, h * LANES : (h + 1) * LANES])
            s.cp[h, here, :LANES] = hi
            s.cp[h, here, LANES:] = lo
        return c

    lax.fori_loop(0, count // SPAN, split, 0)

    def pair(k, h):
        i = h * chips + k
        return remote(s.outp.at[i], s.pair.at[i], s.sb.at[i], s.rb.at[i], other)

    def base(h, share=True):
        def step(dy, dx):
            k = dy * xs + dx
            i = h * chips + k
            for mine_too, side in ((0, 1 - core), (1, core)):
                first = (shard_at(dy, dx, side) * slots).astype(f32)
                one_hot(lambda b: s.uid[b : b + 1, :] - first, lines, s.oh.at[mine_too], slots)
                total = halves(jnp.dot(s.oh[mine_too], s.cp[h], preferred_element_type=f32))
                if mine_too:
                    s.base[i] = total
                else:
                    s.outp[i] = total
                    if share:
                        pair(k, h).start()

        return step

    region("diag", base(0, False))

    loads[3].wait()
    loads[4].wait()
    loads[5].wait()
    s.info[...] = jnp.full_like(s.info, -1)
    s.info[0:1, :batch] = s.owner[...]
    s.info[1:2, :batch] = s.slot[...]
    s.tags[...] = jnp.full_like(s.tags, count)
    pl.semaphore_wait(barrier, zs - 1 + shards - 1)
    region("diag", lambda dy, dx: pair(dy * xs + dx, 0).start())

    order = list(range(zs - 1, 0, -1))
    asked, sent = {}, {}
    for d in order:
        asked[d] = started(s.info, s.mine.at[d], s.si.at[d - 1], s.ri.at[d - 1], mates[d])
    for h in range(parts):
        for d in order:
            here = pl.ds(pl.multiple_of(mates[d]["rows"] * width + h * LANES, LANES), LANES)
            i = h * (zs - 1) + d - 1
            sent[h, d] = started(s.rows.at[:, here], s.slabs.at[h * zs + d], s.ss.at[i], s.rs.at[i], mates[d])
    s.mine[0] = s.info[...]
    for h in range(parts):
        s.slabs[h * zs] = s.rows[:, pl.ds(pl.multiple_of(z * width + h * LANES, LANES), LANES)]

    before = jnp.where(lax.broadcasted_iota(i32, (LANES, LANES), 0) < lane, 1.0, 0.0).astype(bf16)
    shard_of = lax.broadcasted_iota(i32, (shards, LANES), 0)
    spot_of = lax.broadcasted_iota(i32, (spots, LANES), 0)
    line_of = lax.broadcasted_iota(i32, (8, LANES), 0)

    def place(d):
        owner, slot = s.mine[d, 0:1, :], s.mine[d, 1:2, :]
        named = jnp.where(jnp.broadcast_to(owner, (shards, LANES)) == shard_of, 1.0, 0.0)
        earlier = jnp.dot(named.astype(bf16), before, preferred_element_type=f32)
        position = jnp.sum(named * earlier, axis=0, keepdims=True).astype(i32)
        target = jnp.where(owner >= 0, owner * capacity + position, -1)
        pick = jnp.where(jnp.broadcast_to(target, (spots, LANES)) == spot_of, 1.0, 0.0).astype(bf16)
        s.pick[d] = pick
        high = jnp.broadcast_to(lax.shift_right_arithmetic(slot, 7), (8, LANES))
        low = jnp.broadcast_to(slot & 127, (8, LANES))
        code = jnp.where(line_of == 0, high, jnp.where(line_of == 1, low, 1)).astype(f32).astype(bf16)
        found = lax.dot_general(code, pick, (((1,), (1,)), ((), ())), preferred_element_type=f32)
        tag = (found[0:1] * 128.0 + found[1:2]).astype(i32)
        s.tags[d : d + 1, :] = jnp.where(found[2:3] > 0.5, tag, count)

    def spot(p, d):
        return ((p // per) * zs + d) * LANES + (p % per) * capacity

    moves = {}

    def pack(d, h):
        slab = s.slabs[h * zs + d]
        hi, mid = pieces(slab)
        low = (slab - hi.astype(f32) - mid.astype(f32)).astype(bf16)
        three = jnp.concatenate([hi, mid, low], axis=1)
        total = jnp.dot(s.pick[d, :, :batch], three, preferred_element_type=f32)
        total = (total[:, 2 * LANES :] + total[:, LANES : 2 * LANES]) + total[:, :LANES]
        s.packed[h * zs + d] = total
        for p in range(1, shards):
            t = lax.rem(me + p, shards)
            i = ((p - 1) * zs + d) * parts + h
            moves[p, d, h] = started(
                s.packed.at[h * zs + d, pl.ds(pl.multiple_of(t * capacity, 8), capacity)],
                s.inbox.at[h, pl.ds(spot(p, d), capacity)], s.sp.at[i], s.rp.at[i], peers[p],
            )
        s.inbox[h, spot(0, d) : spot(0, d) + capacity, :] = s.packed[
            h * zs + d, pl.ds(pl.multiple_of(me * capacity, 8), capacity), :
        ]

    place(0)
    for h in range(parts):
        pack(0, h)

    region("dy", base(0))

    for d in range(1, zs):
        asked[d].wait_recv()
    for d in range(1, zs):
        place(d)
    told = {p: started(s.tags, s.heard.at[p], s.st.at[p - 1], s.rt.at[p - 1], peers[p]) for p in range(1, shards)}
    s.heard[0] = s.tags[...]

    region("dx", base(0))

    for h in range(parts):
        for d in range(1, zs):
            sent[h, d].wait_recv()
            pack(d, h)

    high = s.own[...] * 8 + lax.div(s.sc[...], block)
    low = lax.rem(s.sc[...], block)
    tile_of = lax.broadcasted_iota(i32, (shards * 8, LANES), 0)
    down = lax.broadcasted_iota(i32, (LANES, LANES), 0)
    for b in range(lines):
        here = slice(b * LANES, (b + 1) * LANES)
        s.ha[:, here] = jnp.where(
            jnp.broadcast_to(high[b : b + 1, :], (shards * 8, LANES)) == tile_of, 1.0, 0.0
        ).astype(bf16)
        s.hb[:, here] = jnp.where(
            jnp.broadcast_to(low[b : b + 1, :], (LANES, LANES)) == down, 1.0, 0.0
        ).astype(bf16)
    s.hist[...] = lax.dot_general(s.ha[...], s.hb[...], (((1,), (1,)), ((), ())), preferred_element_type=f32)
    tallied = {}
    for p in range(1, shards):
        t = lax.rem(me + p, shards)
        tallied[p] = started(
            s.hist.at[pl.ds(pl.multiple_of(t * 8, 8), 8)], s.hs.at[p], s.sh.at[p - 1], s.rh.at[p - 1], peers[p]
        )
    s.hs[0] = s.hist[pl.ds(pl.multiple_of(me * 8, 8), 8), :]

    loads[6].wait()
    for p in range(1, shards):
        told[p].wait_recv()
    few = lax.broadcasted_iota(i32, (s.tags.shape[0], LANES), 1)
    s.lab[...] = jnp.full_like(s.lab, count)
    for g in range(shards // per):
        both = jnp.full(few.shape, count, i32)
        for j in range(per):
            turn = lax.rem((j + shards - me) * capacity, spots)
            turned = pltpu.roll(s.heard[g * per + j], turn, 1)[:, :LANES]
            both = jnp.where((few >= j * capacity) & (few < (j + 1) * capacity), turned, both)
        s.lab[g * zs : (g + 1) * zs, :] = both[:zs].astype(f32)

    band = s.ot.shape[0]

    def gather(jb, c):
        for rr in range(band // LANES):
            r = jb * (band // LANES) + rr
            here = pl.ds(pl.multiple_of(r * LANES, LANES), LANES)
            row = s.lab[pl.ds(r, 1), :]
            label = jnp.broadcast_to(to_column(row, same), (LANES, LANES))

            def alike(q, total):
                return total + jnp.where(label == s.lab[pl.ds(q, 1), :], 1.0, 0.0)

            mates_of = lax.fori_loop(0, across, alike, jnp.zeros((LANES, LANES), f32), unroll=min(across, 4))
            had, named = jnp.zeros((LANES, LANES), f32), jnp.zeros((LANES, LANES), f32)
            for b in range(lines):
                hit = label == (lane + b * LANES).astype(f32)
                s.ot[rr * LANES : (rr + 1) * LANES, b * LANES : (b + 1) * LANES] = jnp.where(hit, 1.0, 0.0).astype(bf16)
                had = had + jnp.where(hit, s.counts[b : b + 1, :], 0.0)
                named = named + jnp.where(hit, s.uid[b : b + 1, :], 0.0)
            n = jnp.sum(had + mates_of, axis=1, keepdims=True)
            s.share[here, :] = jnp.broadcast_to(1.0 / n, (LANES, LANES))
            target = to_row(jnp.sum(named, axis=1, keepdims=True), same)
            s.urow[pl.ds(r, 1), :] = jnp.where(row < float(count), target, -1.0)
        for h in range(parts):
            s.near[h, pl.ds(pl.multiple_of(jb * band, band), band), :] = halves(
                jnp.dot(s.ot[...], s.cp[h], preferred_element_type=f32)
            )
        return c

    s.urow[...] = jnp.full_like(s.urow, -1.0)
    each(joined // band, lambda jb: gather(jb, 0))
    linked = started(s.urow, s.prow, s.su.at[0], s.ru.at[0], other)

    def give(h):
        return remote(s.dl.at[h], s.pd.at[h], s.sd.at[h], s.rd.at[h], other)

    def change(h):
        for p in range(1, shards):
            for d in range(zs):
                moves[p, d, h].wait_recv()

        def step(e):
            here = pl.ds(e * SPAN, SPAN)
            s.dl[h, here, :] = (s.inbox[h, here, :] - s.near[h, here, :]) * s.share[here, :]

        each(joined // SPAN, step)
        give(h).start()

        def cut(e):
            here = pl.ds(e * SPAN, SPAN)
            hi, lo = pieces(s.dl[h, here, :])
            s.dd[h, here, :LANES] = hi
            s.dd[h, here, LANES:] = lo

        each(joined // SPAN, cut)

    def accept(h):
        give(h).wait_recv()

        def cut(e):
            here = pl.ds(e * SPAN, SPAN)
            there = pl.ds(e * SPAN + joined, SPAN)
            hi, lo = pieces(s.pd[h, here, :])
            s.dd[h, there, :LANES] = hi
            s.dd[h, there, LANES:] = lo

        each(joined // SPAN, cut)

    def at(dy, dx):
        return lax.rem(y + dy, ys), lax.rem(x + dx, xs)

    na, nb = (ys - 1) * xs, (xs - 1) * ys

    def a1(dy, dx, h):
        i = h * na + (dy - 1) * xs + dx
        return remote(
            s.chip.at[h * chips + dy * xs + dx, pl.ds(0, half)], s.a1.at[i], s.sa1.at[i], s.ra1.at[i],
            {"cx": lax.rem(y + dy, ys), "cy": cy},
        )

    def b1(dy, dx, h):
        i = h * nb + (dx - 1) * ys + dy
        return remote(
            s.chip.at[h * chips + dy * xs + dx, pl.ds(half, half)], s.b1.at[i], s.sb1.at[i], s.rb1.at[i],
            {"cx": y, "cy": lax.rem(x + dx, xs) * CORES + core},
        )

    def a2(dx, h):
        i = h * (xs - 1) + dx - 1
        return remote(
            s.relay_a.at[i], s.a2.at[i], s.sa2.at[i], s.ra2.at[i],
            {"cx": y, "cy": lax.rem(x + dx, xs) * CORES + core},
        )

    def b2(dy, h):
        i = h * (ys - 1) + dy - 1
        return remote(
            s.relay_b.at[i], s.b2.at[i], s.sb2.at[i], s.rb2.at[i],
            {"cx": lax.rem(y + dy, ys), "cy": cy},
        )

    def combine(h, name):
        def step(dy, dx):
            k = dy * xs + dx
            i = h * chips + k
            first = (shard_at(dy, dx, core) * slots).astype(f32)
            one_hot(
                lambda b: (s.urow[b : b + 1, :] if b < across else s.prow[b - across : b - across + 1, :]) - first,
                2 * across, s.oh3, slots,
            )
            pair(k, h).wait_recv()
            total = halves(jnp.dot(s.oh3[...], s.dd[h], preferred_element_type=f32))
            s.chip[i] = total + (s.base[i] + s.pair[i])
            if name in ("diag", "dy"):
                a1(dy, dx, h).start()
            if name in ("diag", "dx"):
                b1(dy, dx, h).start()

        region(name, step)

    def forward(h):
        for dx in range(1, xs):
            i = h * chips + dx
            total = s.chip[i, :half]
            for dy in range(1, ys):
                a1(dy, dx, h).wait_recv()
                total = total + s.a1[h * na + (dy - 1) * xs + dx]
            s.relay_a[h * (xs - 1) + dx - 1] = total
            a2(dx, h).start()
        for dy in range(1, ys):
            i = h * chips + dy * xs
            total = s.chip[i, half:]
            for dx in range(1, xs):
                b1(dy, dx, h).wait_recv()
                total = total + s.b1[h * nb + (dx - 1) * ys + dy]
            s.relay_b[h * (ys - 1) + dy - 1] = total
            b2(dy, h).start()

    change(0)
    for h in range(1, parts):
        region("diag", base(h))
    linked.wait_recv()
    accept(0)
    for name in ("diag", "dy", "dx"):
        combine(0, name)
    for h in range(1, parts):
        region("dy", base(h))
        region("dx", base(h))
        change(h)
        if h == 1:
            region("own", base(0))
        accept(h)
        for name in ("diag", "dy", "dx"):
            combine(h, name)
    if parts == 1:
        region("own", base(0))
    combine(0, "own")
    forward(0)

    loads[7].wait()
    loads[8].wait()

    def lay(e):
        here = pl.ds(e * SPAN, SPAN)
        for h in range(parts):
            hi, lo = pieces(s.inbox[h, here, :])
            s.dp[here, 2 * h * LANES : (2 * h + 1) * LANES] = hi
            s.dp[here, (2 * h + 1) * LANES : (2 * h + 2) * LANES] = lo
        s.dp[here, 2 * parts * LANES :] = jnp.ones((SPAN, LANES), bf16)

    each(joined // SPAN, lay)

    def move(e):
        first = (jnp.int32(e) * height).astype(f32)
        one_hot(lambda b: s.lab[b : b + 1, :] - first, across, s.oh1, height)
        s.sums[...] = jnp.dot(s.oh1[...], s.dp[...], preferred_element_type=f32)
        for sub in range(height // LANES):
            b = e * (height // LANES) + sub
            here = pl.ds(pl.multiple_of(b * LANES, LANES), LANES)
            local = slice(sub * LANES, (sub + 1) * LANES)
            m = s.sums[local, 2 * parts * LANES :]
            n = to_column(s.counts[pl.ds(b, 1), :], same) + m
            r = 1.0 / n
            for h in range(parts):
                total = s.sums[local, 2 * h * LANES : (2 * h + 1) * LANES] + s.sums[
                    local, (2 * h + 1) * LANES : (2 * h + 2) * LANES
                ]
                old = s.cent[here, h * LANES : (h + 1) * LANES]
                moved[here, h * LANES : (h + 1) * LANES] = old + (total - m * old) * r
            news[pl.ds(b, 1), :] = to_row(n, same)

    each(count // height, move)

    for h in range(1, parts):
        region("own", base(h))
        combine(h, "own")
        forward(h)

    tally = s.hs[0]
    for p in range(1, shards):
        tallied[p].wait_recv()
        tally = tally + s.hs[p]
    members = tally[:tall, :block]
    upnews[...] = s.weights[...] + members
    square_block = square(block)

    def finish(h):
        base_i = h * chips
        for dy in range(1, ys):
            a1(dy, 0, h).wait_recv()
        for dx in range(1, xs):
            b1(0, dx, h).wait_recv()
        for dx in range(1, xs):
            a2(dx, h).wait_recv()
        for dy in range(1, ys):
            b2(dy, h).wait_recv()
        total = s.chip[base_i, :half]
        for dy in range(1, ys):
            total = total + s.a1[h * na + (dy - 1) * xs]
        for dx in range(1, xs):
            total = total + s.a2[h * (xs - 1) + dx - 1]
        s.fin[:half] = total
        total = s.chip[base_i, half:]
        for dx in range(1, xs):
            total = total + s.b1[h * nb + (dx - 1) * ys]
        for dy in range(1, ys):
            total = total + s.b2[h * (ys - 1) + dy - 1]
        s.fin[half:] = total
        for line in range(tall):
            here = slice(line * block, (line + 1) * block)
            m = to_column(members[line : line + 1, :], square_block)
            n = to_column(s.weights[line : line + 1, :], square_block) + m
            prev = s.upper[here, h * LANES : (h + 1) * LANES]
            newup[here, h * LANES : (h + 1) * LANES] = prev + (s.fin[here, :] - m * prev) / n

    for h in range(parts):
        finish(h)

    for copy in list(asked.values()) + list(sent.values()) + list(moves.values()):
        copy.wait_send()
    for copy in list(told.values()) + list(tallied.values()) + [linked]:
        copy.wait_send()
    each(parts * chips, lambda i: pair(jnp.int32(i), 0).wait_send())
    for h in range(parts):
        give(h).wait_send()
        for name in ("diag", "dy"):
            region(name, lambda dy, dx: a1(dy, dx, h).wait_send())
        for name in ("diag", "dx"):
            region(name, lambda dy, dx: b1(dy, dx, h).wait_send())
        for dx in range(1, xs):
            a2(dx, h).wait_send()
        for dy in range(1, ys):
            b2(dy, h).wait_send()


def emit_kernel(moved_v, news_v, up_v, upnews_v, moved, news, up, upnews, sems):
    copies = [
        pltpu.make_async_copy(src, dst, sems.at[i])
        for i, (src, dst) in enumerate(((moved_v, moved), (up_v, up), (news_v, news), (upnews_v, upnews)))
    ]
    for copy in copies:
        copy.start()
    for copy in copies:
        copy.wait()


def body(
    rows_data, owner_rows, slot_rows, centroids, counts, owner_cent, slot_cent, upper, upper_counts
):
    zs, ys, xs = lax.axis_size("rows"), lax.axis_size("cx"), lax.axis_size("cy") // CORES
    chips = ys * xs
    shards = chips * CORES
    batch, features = rows_data.shape
    count, width = centroids.shape
    parts = width // LANES
    slots = upper.shape[0]
    half = slots // 2
    block = min(LANES, slots)
    capacity = -(-(2 * batch // shards) // 8) * 8
    spots = shards * capacity
    across = zs * spots // LANES
    joined = across * LANES
    tall = -(-zs // 8) * 8
    padded = -(-across // 8) * 8
    band = min(joined, 512)
    height = min(count, 512)
    na, nb = (ys - 1) * xs, (xs - 1) * ys

    vm = pl.BlockSpec(memory_space=pltpu.VMEM)
    hbm = pl.BlockSpec(memory_space=pl.ANY)
    V = pltpu.VMEM
    dma = lambda n: pltpu.SemaphoreType.DMA((n,))
    scratch = dict(
        oc=V((1, count), i32), sc=V((count // LANES, LANES), i32), cent=V((count, width), f32),
        owner=V((1, batch), i32), slot=V((1, batch), i32), rows=V((batch, features), f32),
        counts=V((count // LANES, LANES), f32), upper=V((slots, width), f32),
        weights=V((slots // block, block), f32),
        own=V((count // LANES, LANES), i32), uid=V((count // LANES, LANES), f32),
        cp=V((parts, count, 2 * LANES), bf16), oh=V((2, slots, count), bf16),
        outp=V((parts * chips, slots, LANES), f32), pair=V((parts * chips, slots, LANES), f32),
        base=V((parts * chips, slots, LANES), f32), chip=V((parts * chips, slots, LANES), f32),
        info=V((8, LANES), i32), mine=V((zs, 8, LANES), i32),
        slabs=V((parts * zs, batch, LANES), f32), pick=V((zs, spots, LANES), bf16),
        packed=V((parts * zs, spots, LANES), f32), inbox=V((parts, joined, LANES), f32),
        tags=V((tall, spots), i32), heard=V((shards, tall, spots), i32),
        ha=V((shards * 8, count), bf16), hb=V((LANES, count), bf16), hist=V((shards * 8, LANES), f32),
        hs=V((shards, 8, LANES), f32), lab=V((padded, LANES), f32), urow=V((padded, LANES), f32),
        prow=V((padded, LANES), f32), ot=V((band, count), bf16), share=V((joined, LANES), f32),
        near=V((parts, joined, LANES), f32), dl=V((parts, joined, LANES), f32),
        pd=V((parts, joined, LANES), f32), dd=V((parts, 2 * joined, 2 * LANES), bf16),
        oh3=V((slots, 2 * joined), bf16),
        a1=V((parts * na, half, LANES), f32), b1=V((parts * nb, half, LANES), f32),
        a2=V((parts * (xs - 1), half, LANES), f32), b2=V((parts * (ys - 1), half, LANES), f32),
        relay_a=V((parts * (xs - 1), half, LANES), f32), relay_b=V((parts * (ys - 1), half, LANES), f32),
        dp=V((joined, (2 * parts + 1) * LANES), bf16), oh1=V((height, joined), bf16),
        sums=V((height, (2 * parts + 1) * LANES), f32), fin=V((slots, LANES), f32),
        ld=dma(9), si=dma(zs - 1), ri=dma(zs - 1), ss=dma(parts * (zs - 1)), rs=dma(parts * (zs - 1)),
        sp=dma((shards - 1) * zs * parts), rp=dma((shards - 1) * zs * parts),
        st=dma(shards - 1), rt=dma(shards - 1), sh=dma(shards - 1), rh=dma(shards - 1),
        sb=dma(parts * chips), rb=dma(parts * chips), su=dma(1), ru=dma(1), sd=dma(parts), rd=dma(parts),
        sa1=dma(parts * na), ra1=dma(parts * na), sb1=dma(parts * nb), rb1=dma(parts * nb),
        sa2=dma(parts * (xs - 1)), ra2=dma(parts * (xs - 1)), sb2=dma(parts * (ys - 1)), rb2=dma(parts * (ys - 1)),
    )
    outs = (
        jax.ShapeDtypeStruct((count, width), f32),
        jax.ShapeDtypeStruct((count // LANES, LANES), f32),
        jax.ShapeDtypeStruct((slots, width), f32),
        jax.ShapeDtypeStruct((slots // block, block), f32),
    )
    made = pl.pallas_call(
        functools.partial(fused_kernel, tuple(scratch), (zs, ys, xs, capacity, height)),
        out_shape=outs,
        in_specs=[pl.BlockSpec(memory_space=pltpu.HBM)] * 9,
        out_specs=(vm,) * 4,
        scratch_shapes=list(scratch.values()),
        compiler_params=pltpu.CompilerParams(
            collective_id=1, has_side_effects=True, vmem_limit_bytes=44 * 1024 * 1024
        ),
        name="update",
    )(*[pltpu.with_memory_space_constraint(a, pltpu.HBM) for a in (
        rows_data, owner_rows.reshape(1, batch), slot_rows.reshape(1, batch), centroids,
        counts.reshape(-1, LANES), owner_cent.reshape(1, count), slot_cent.reshape(-1, LANES),
        upper, upper_counts.reshape(-1, block),
    )])
    moved, news, new_upper, upnews = pl.pallas_call(
        emit_kernel,
        out_shape=outs,
        in_specs=[vm] * 4,
        out_specs=(hbm,) * 4,
        scratch_shapes=[dma(4)],
        compiler_params=pltpu.CompilerParams(vmem_limit_bytes=4 * 1024 * 1024),
        name="emit",
    )(*made)
    return moved, news.reshape(-1), new_upper, upnews.reshape(-1)


def solution(mesh):
    placed = (
        P(("rows", "cx", "cy"), None),
        P(("rows", "cx", "cy"), None),
        P(("rows", "cx", "cy")),
        P(("cx", "cy"), "rows"),
        P(("cx", "cy")),
        P(("cx", "cy"), None),
        P(("cx", "cy")),
        P(("cx", "cy"), "rows"),
        P(("cx", "cy")),
    )
    return jax.shard_map(
        body,
        mesh=mesh,
        in_specs=placed,
        out_specs=(
            P(("cx", "cy"), "rows"),
            P(("cx", "cy")),
            P(("cx", "cy"), "rows"),
            P(("cx", "cy")),
        ),
        check_vma=False,
    )
```

```python
import functools
import types

import jax
import jax.numpy as jnp
from jax import lax
from jax.experimental import pallas as pl
from jax.experimental.pallas import tpu as pltpu
from jax.sharding import PartitionSpec as P

MESH = pl.DeviceIdType.MESH
LANES = 128
CORES = 2
SPAN = 256
bf16, f32, i32 = jnp.bfloat16, jnp.float32, jnp.int32


def pieces(x):
    first = x.astype(bf16)
    return first, (x - first.astype(f32)).astype(bf16)


def halves(x):
    return x[:, :LANES] + x[:, LANES : 2 * LANES]


def square(size):
    up = lax.broadcasted_iota(i32, (size, size), 0)
    return up == lax.broadcasted_iota(i32, (size, size), 1)


def to_column(row, same):
    size = row.shape[1]
    return jnp.sum(jnp.where(same, jnp.broadcast_to(row, (size, size)), 0.0), axis=1, keepdims=True)


def to_row(column, same):
    return jnp.sum(jnp.where(same, jnp.broadcast_to(column, same.shape), 0.0), axis=0, keepdims=True)


def each(count, step):
    if count == 1:
        step(0)
    elif count > 1:
        lax.fori_loop(0, count, lambda e, c: (step(e), c)[1], 0)


def one_hot(row_of, lines, out, height):
    span = min(SPAN, height)
    spots = lax.broadcasted_iota(i32, (span, LANES), 0).astype(f32).astype(bf16)
    one, zero = jnp.ones((span, LANES), bf16), jnp.zeros((span, LANES), bf16)
    for q in range(height // span):
        for b in range(lines):
            row = jnp.broadcast_to(row_of(b) - float(q * span), (16, LANES)).astype(bf16)
            row = jnp.concatenate([row] * (span // 16), axis=0)
            out[q * span : (q + 1) * span, b * LANES : (b + 1) * LANES] = jnp.where(row == spots, one, zero)


def fused_kernel(
    names, sizes, rows_h, owner_h, slot_h, cent_h, counts_h, oc_h, sc_h, upper_h, weights_h,
    moved, news, newup, upnews, *scratch,
):
    s = types.SimpleNamespace(**dict(zip(names, scratch)))
    zs, ys, xs, capacity, height = sizes
    chips, cys = ys * xs, xs * CORES
    shards = chips * CORES
    batch = rows_h.shape[0]
    count, width = cent_h.shape
    parts = width // LANES
    lines = count // LANES
    slots = upper_h.shape[0]
    half = slots // 2
    tall, block = weights_h.shape
    spots = shards * capacity
    per = LANES // capacity
    across = zs * spots // LANES
    joined = across * LANES

    z, y, cy = lax.axis_index("rows"), lax.axis_index("cx"), lax.axis_index("cy")
    x, core = lax.div(cy, CORES), lax.rem(cy, CORES)
    me = y * cys + cy
    other = {"cx": y, "cy": x * CORES + 1 - core}

    def mate(d):
        if zs & (zs - 1):
            return lax.rem(z + d, zs)
        at = z
        bit = 1
        while bit <= d:
            if d & bit:
                at = at + bit * (1 - 2 * lax.rem(lax.div(z, bit), 2))
            bit *= 2
        return at

    mates = {d: {"rows": mate(d)} for d in range(1, zs)}
    peers = {}
    for p in range(1, shards):
        t = lax.rem(me + p, shards)
        peers[p] = {"cx": lax.div(t, cys), "cy": lax.rem(t, cys)}

    barrier = pltpu.get_barrier_semaphore()
    for peer in list(mates.values()) + list(peers.values()):
        pl.semaphore_signal(barrier, inc=1, device_id=peer, device_id_type=MESH)

    loads = [
        pltpu.make_async_copy(src, dst, s.ld.at[i])
        for i, (src, dst) in enumerate([
            (owner_h, s.owner), (slot_h, s.slot), (rows_h, s.rows), (oc_h, s.oc), (sc_h, s.sc),
            (cent_h, s.cent), (counts_h, s.counts), (upper_h, s.upper), (weights_h, s.weights),
        ])
    ]
    for copy in loads:
        copy.start()

    def remote(src, dst, send, recv, peer):
        return pltpu.make_async_remote_copy(
            src_ref=src, dst_ref=dst, send_sem=send, recv_sem=recv, device_id=peer, device_id_type=MESH
        )

    def started(*args):
        copy = remote(*args)
        copy.start()
        return copy

    same = square(LANES)
    lane = lax.broadcasted_iota(i32, (LANES, LANES), 1)

    regions = {
        "diag": ((ys - 1) * (xs - 1), lambda e: (1 + lax.div(e, xs - 1), 1 + lax.rem(e, xs - 1))),
        "dy": (ys - 1, lambda e: (1 + e, 0)),
        "dx": (xs - 1, lambda e: (0, 1 + e)),
        "own": (1, lambda e: (0, 0)),
    }

    def region(name, step):
        number, where = regions[name]

        def run(e):
            if isinstance(e, int):
                e = jnp.int32(e)
            step(*where(e))

        each(number, run)

    def shard_at(dy, dx, side):
        return (lax.rem(y + dy, ys) * xs + lax.rem(x + dx, xs)) * CORES + side

    loads[0].wait()
    loads[1].wait()
    loads[2].wait()
    s.info[...] = jnp.full_like(s.info, -1)
    s.info[0:1, :batch] = s.owner[...]
    s.info[1:2, :batch] = s.slot[...]
    s.tags[...] = jnp.full_like(s.tags, count)
    pl.semaphore_wait(barrier, zs - 1 + shards - 1)

    targets = []
    low_end, high_end = jnp.int32(0), jnp.int32(zs - 1)
    for _ in range(1, zs):
        under, over = z - low_end, high_end - z
        take = (under > over) | ((under == over) & (2 * z < zs))
        targets.append(jnp.where(take, low_end, high_end))
        low_end = low_end + jnp.where(take, 1, 0)
        high_end = high_end - jnp.where(take, 0, 1)

    def place_of(t):
        if zs & (zs - 1):
            return lax.rem(t - z + zs, zs)
        total, bit = 0, 1
        while bit < zs:
            total = total + bit * lax.rem(lax.div(z, bit) + lax.div(t, bit), 2)
            bit *= 2
        return total

    def ask(d, t):
        return remote(s.info, s.mine.at[d], s.si.at[d - 1], s.ri.at[d - 1], {"rows": t})

    def slab(d, t, h):
        here = pl.ds(pl.multiple_of(t * width + h * LANES, LANES), LANES)
        i = h * (zs - 1) + d - 1
        return remote(s.rows.at[:, here], s.slabs.at[h * zs + d], s.ss.at[i], s.rs.at[i], {"rows": t})

    asked = {d: ask(d, mates[d]["rows"]) for d in range(1, zs)}
    sent = {(h, d): slab(d, mates[d]["rows"], h) for h in range(parts) for d in range(1, zs)}
    for t in targets:
        ask(place_of(t), t).start()

    def scatter(h):
        for t in targets:
            slab(place_of(t), t, h).start()

    scatter(0)
    s.mine[0] = s.info[...]
    for h in range(parts):
        s.slabs[h * zs] = s.rows[:, pl.ds(pl.multiple_of(z * width + h * LANES, LANES), LANES)]

    before = jnp.where(lax.broadcasted_iota(i32, (LANES, LANES), 0) < lane, 1.0, 0.0).astype(bf16)
    shard_of = lax.broadcasted_iota(i32, (shards, LANES), 0)
    spot_of = lax.broadcasted_iota(i32, (spots, LANES), 0)
    line_of = lax.broadcasted_iota(i32, (8, LANES), 0)

    def place(d):
        owner, slot = s.mine[d, 0:1, :], s.mine[d, 1:2, :]
        named = jnp.where(jnp.broadcast_to(owner, (shards, LANES)) == shard_of, 1.0, 0.0)
        earlier = jnp.dot(named.astype(bf16), before, preferred_element_type=f32)
        position = jnp.sum(named * earlier, axis=0, keepdims=True).astype(i32)
        target = jnp.where(owner >= 0, owner * capacity + position, -1)
        pick = jnp.where(jnp.broadcast_to(target, (spots, LANES)) == spot_of, 1.0, 0.0).astype(bf16)
        s.pick[d] = pick
        high = jnp.broadcast_to(lax.shift_right_arithmetic(slot, 7), (8, LANES))
        low = jnp.broadcast_to(slot & 127, (8, LANES))
        code = jnp.where(line_of == 0, high, jnp.where(line_of == 1, low, 1)).astype(f32).astype(bf16)
        found = lax.dot_general(code, pick, (((1,), (1,)), ((), ())), preferred_element_type=f32)
        tag = (found[0:1] * 128.0 + found[1:2]).astype(i32)
        s.tags[d : d + 1, :] = jnp.where(found[2:3] > 0.5, tag, count)

    def spot(p, d):
        return ((p // per) * zs + d) * LANES + (p % per) * capacity

    moves = {}

    def pack(d, h):
        slab = s.slabs[h * zs + d]
        hi, mid = pieces(slab)
        low = (slab - hi.astype(f32) - mid.astype(f32)).astype(bf16)
        three = jnp.concatenate([hi, mid, low], axis=1)
        total = jnp.dot(s.pick[d, :, :batch], three, preferred_element_type=f32)
        total = (total[:, 2 * LANES :] + total[:, LANES : 2 * LANES]) + total[:, :LANES]
        s.packed[h * zs + d] = total

    def post(d, h):
        for p in range(1, shards):
            t = lax.rem(me + p, shards)
            i = ((p - 1) * zs + d) * parts + h
            moves[p, d, h] = started(
                s.packed.at[h * zs + d, pl.ds(pl.multiple_of(t * capacity, 8), capacity)],
                s.inbox.at[h, pl.ds(spot(p, d), capacity)], s.sp.at[i], s.rp.at[i], peers[p],
            )

    def keep(d, h):
        s.inbox[h, spot(0, d) : spot(0, d) + capacity, :] = s.packed[
            h * zs + d, pl.ds(pl.multiple_of(me * capacity, 8), capacity), :
        ]

    place(0)
    for h in range(parts):
        pack(0, h)
    for h in range(parts):
        post(0, h)
        keep(0, h)

    loads[3].wait()
    loads[4].wait()
    for b in range(lines):
        s.own[b : b + 1, :] = s.oc[0:1, b * LANES : (b + 1) * LANES]
    s.uid[...] = (s.own[...] * slots + s.sc[...]).astype(f32)
    loads[5].wait()

    def split(b, c):
        here = pl.ds(pl.multiple_of(b * SPAN, SPAN), SPAN)
        for h in range(parts):
            hi, lo = pieces(s.cent[here, h * LANES : (h + 1) * LANES])
            s.cp[h, here, :LANES] = hi
            s.cp[h, here, LANES:] = lo
        return c

    lax.fori_loop(0, count // SPAN, split, 0)
    loads[6].wait()
    s.tab[...] = jnp.zeros_like(s.tab)
    near_c, mid_c = pieces(s.counts[...])
    far_c = (s.counts[...] - near_c.astype(f32) - mid_c.astype(f32)).astype(bf16)
    for i, part in enumerate((near_c, mid_c, far_c) + pieces(s.uid[...])):
        s.tab[:lines, i * LANES : (i + 1) * LANES] = part

    def pair(k, h):
        i = h * chips + k
        return remote(s.outp.at[i], s.pair.at[i], s.sb.at[i], s.rb.at[i], other)

    def base(h):
        def step(dy, dx):
            k = dy * xs + dx
            i = h * chips + k
            for mine_too, side in ((0, 1 - core), (1, core)):
                first = (shard_at(dy, dx, side) * slots).astype(f32)
                one_hot(lambda b: s.uid[b : b + 1, :] - first, lines, s.oh.at[mine_too], slots)
                total = halves(jnp.dot(s.oh[mine_too], s.cp[h], preferred_element_type=f32))
                if mine_too:
                    s.base[i] = total
                else:
                    s.outp[i] = total
            pair(k, h).start()

        return step

    region("diag", base(0))
    for h in range(1, parts):
        scatter(h)
    region("dy", base(0))

    for d in range(1, zs):
        asked[d].wait_recv()
    for d in range(1, zs):
        place(d)
    told = {p: started(s.tags, s.heard.at[p], s.st.at[p - 1], s.rt.at[p - 1], peers[p]) for p in range(1, shards)}
    s.heard[0] = s.tags[...]

    def relay(h):
        for d in range(1, zs):
            sent[h, d].wait_recv()
        for d in range(1, zs):
            pack(d, h)
        for d in range(1, zs):
            post(d, h)

    for d in range(1, zs):
        if d == zs - 1:
            region("dx", base(0))
        sent[0, d].wait_recv()
        pack(d, 0)
        post(d, 0)
    for d in range(1, zs):
        keep(d, 0)

    for p in range(1, shards):
        told[p].wait_recv()
    few = lax.broadcasted_iota(i32, (s.tags.shape[0], LANES), 1)
    s.lab[...] = jnp.full_like(s.lab, count)
    for g in range(shards // per):
        both = jnp.full(few.shape, count, i32)
        for j in range(per):
            turn = lax.rem((j + shards - me) * capacity, spots)
            turned = pltpu.roll(s.heard[g * per + j], turn, 1)[:, :LANES]
            both = jnp.where((few >= j * capacity) & (few < (j + 1) * capacity), turned, both)
        s.lab[g * zs : (g + 1) * zs, :] = both[:zs].astype(f32)

    band = s.ot.shape[0]

    def fetch(jb, h):
        here = pl.ds(pl.multiple_of(jb * band, band), band)
        s.near[h, here, :] = halves(jnp.dot(s.ot[...], s.cp[h], preferred_element_type=f32))

    across_f = lane.astype(f32)
    across_h = across_f.astype(bf16)
    unit, none = jnp.ones((LANES, LANES), bf16), jnp.zeros((LANES, LANES), bf16)

    def gather(jb):
        for rr in range(band // LANES):
            r = jb * (band // LANES) + rr
            here = pl.ds(pl.multiple_of(r * LANES, LANES), LANES)
            row = s.lab[pl.ds(r, 1), :]
            column = to_column(row, same)
            top = jnp.floor(column * (1.0 / LANES))
            label = jnp.broadcast_to(column, (LANES, LANES))
            major = jnp.broadcast_to(top, (LANES, LANES))
            minor = jnp.broadcast_to(column - top * float(LANES), (LANES, LANES))

            def alike(q, total):
                return total + jnp.where(label == s.lab[pl.ds(q, 1), :], 1.0, 0.0)

            total = jnp.zeros((LANES, LANES), f32)
            if across <= 8:
                for q in range(across):
                    total = alike(q, total)
            else:
                total = lax.fori_loop(0, across, alike, total)
            line_at = jnp.where(across_f == major, 1.0, 0.0).astype(bf16)
            found = jnp.dot(line_at, s.tab[...], preferred_element_type=f32)
            had = (found[:, :LANES] + found[:, LANES : 2 * LANES]) + found[:, 2 * LANES : 3 * LANES]
            named = found[:, 3 * LANES : 4 * LANES] + found[:, 4 * LANES :]
            hit = across_f == minor
            n = jnp.sum(jnp.where(hit, had, 0.0) + total, axis=1, keepdims=True)
            s.share[here, :] = jnp.broadcast_to(1.0 / n, (LANES, LANES))
            target = to_row(jnp.sum(jnp.where(hit, named, 0.0), axis=1, keepdims=True), same)
            s.urow[pl.ds(r, 1), :] = jnp.where(row < float(count), target, -1.0)
            spread = jnp.where(minor.astype(bf16) == across_h, unit, none)
            major_h = major.astype(bf16)
            for b in range(lines):
                s.ot[rr * LANES : (rr + 1) * LANES, b * LANES : (b + 1) * LANES] = jnp.where(
                    major_h == jnp.full((LANES, LANES), float(b), bf16), spread, none
                )
        for h in range(parts if joined > band else 1):
            fetch(jb, h)

    s.urow[...] = jnp.full_like(s.urow, -1.0)
    each(joined // band, gather)
    linked = started(s.urow, s.prow, s.su.at[0], s.ru.at[0], other)
    ready = parts > 1

    def aim(rows, begin):
        def step(dy, dx):
            k = (dy * xs + dx) if ready else 0
            first = (shard_at(dy, dx, core) * slots).astype(f32)
            one_hot(
                lambda b: rows[b : b + 1, :] - first, across, s.oh3.at[k, :, pl.ds(begin, joined)], slots
            )

        return step

    if ready:
        for name in ("diag", "dy", "dx"):
            region(name, aim(s.urow, 0))
    linked.wait_recv()
    if ready:
        for name in ("diag", "dy", "dx"):
            region(name, aim(s.prow, joined))

    for h in range(1, parts):
        relay(h)
        for d in range(1, zs):
            keep(d, h)

    def give(h):
        return remote(s.dl.at[h], s.pd.at[h], s.sd.at[h], s.rd.at[h], other)

    def change(h):
        for p in range(1, shards):
            for d in range(zs):
                moves[p, d, h].wait_recv()

        def step(e):
            here = pl.ds(e * SPAN, SPAN)
            s.dl[h, here, :] = (s.inbox[h, here, :] - s.near[h, here, :]) * s.share[here, :]

        each(joined // SPAN, step)
        give(h).start()

        def cut(e):
            here = pl.ds(e * SPAN, SPAN)
            hi, lo = pieces(s.dl[h, here, :])
            s.dd[h, here, :LANES] = hi
            s.dd[h, here, LANES:] = lo

        each(joined // SPAN, cut)

    def accept(h):
        give(h).wait_recv()

        def cut(e):
            here = pl.ds(e * SPAN, SPAN)
            there = pl.ds(e * SPAN + joined, SPAN)
            hi, lo = pieces(s.pd[h, here, :])
            s.dd[h, there, :LANES] = hi
            s.dd[h, there, LANES:] = lo

        each(joined // SPAN, cut)

    def at(dy, dx):
        return lax.rem(y + dy, ys), lax.rem(x + dx, xs)

    na, nb = (ys - 1) * xs, (xs - 1) * ys

    def a1(dy, dx, h):
        i = h * na + (dy - 1) * xs + dx
        return remote(
            s.chip.at[h * chips + dy * xs + dx, pl.ds(0, half)], s.a1.at[i], s.sa1.at[i], s.ra1.at[i],
            {"cx": lax.rem(y + dy, ys), "cy": cy},
        )

    def b1(dy, dx, h):
        i = h * nb + (dx - 1) * ys + dy
        return remote(
            s.chip.at[h * chips + dy * xs + dx, pl.ds(half, half)], s.b1.at[i], s.sb1.at[i], s.rb1.at[i],
            {"cx": y, "cy": lax.rem(x + dx, xs) * CORES + core},
        )

    def a2(dx, h):
        i = h * (xs - 1) + dx - 1
        return remote(
            s.relay_a.at[i], s.a2.at[i], s.sa2.at[i], s.ra2.at[i],
            {"cx": y, "cy": lax.rem(x + dx, xs) * CORES + core},
        )

    def b2(dy, h):
        i = h * (ys - 1) + dy - 1
        return remote(
            s.relay_b.at[i], s.b2.at[i], s.sb2.at[i], s.rb2.at[i],
            {"cx": lax.rem(y + dy, ys), "cy": cy},
        )

    def prepare(h):
        def step(dy, dx):
            k = dy * xs + dx
            i = h * chips + k
            o = k if ready else 0
            if not ready:
                aim(s.urow, 0)(dy, dx)
                aim(s.prow, joined)(dy, dx)
            pair(k, h).wait_recv()
            total = halves(jnp.dot(s.oh3[o, :, :joined], s.dd[h, :joined, :], preferred_element_type=f32))
            s.chip[i] = total + (s.base[i] + s.pair[i])

        return step

    def combine(h, name):
        def step(dy, dx):
            k = dy * xs + dx
            i = h * chips + k
            o = k if ready else 0
            if not ready:
                prepare(h)(dy, dx)
            total = halves(jnp.dot(s.oh3[o, :, joined:], s.dd[h, joined:, :], preferred_element_type=f32))
            s.chip[i] = s.chip[i] + total
            if name in ("diag", "dy"):
                a1(dy, dx, h).start()
            if name in ("diag", "dx"):
                b1(dy, dx, h).start()

        region(name, step)

    def ahead(h, names):
        if ready:
            for name in names:
                region(name, prepare(h))

    def forward(h):
        for dx in range(1, xs):
            i = h * chips + dx
            total = s.chip[i, :half]
            for dy in range(1, ys):
                a1(dy, dx, h).wait_recv()
                total = total + s.a1[h * na + (dy - 1) * xs + dx]
            s.relay_a[h * (xs - 1) + dx - 1] = total
            a2(dx, h).start()
        for dy in range(1, ys):
            i = h * chips + dy * xs
            total = s.chip[i, half:]
            for dx in range(1, xs):
                b1(dy, dx, h).wait_recv()
                total = total + s.b1[h * nb + (dx - 1) * ys + dy]
            s.relay_b[h * (ys - 1) + dy - 1] = total
            b2(dy, h).start()

    change(0)
    ahead(0, ("diag", "dy", "dx"))
    accept(0)
    for name in ("diag", "dy", "dx"):
        combine(0, name)
    for h in range(1, parts):
        if joined <= band:
            fetch(0, h)
        region("diag", base(h))
        region("dy", base(h))
        region("dx", base(h))
        if h == 1:
            forward(0)
        change(h)
        ahead(h, ("diag", "dy", "dx"))
        accept(h)
        for name in ("diag", "dy", "dx"):
            combine(h, name)
    if parts == 1:
        forward(0)
    region("own", base(0))
    if ready:
        region("own", aim(s.urow, 0))
        region("own", aim(s.prow, joined))
    ahead(0, ("own",))
    combine(0, "own")

    high = s.own[...] * 8 + lax.div(s.sc[...], block)
    low = lax.rem(s.sc[...], block)
    tile_of = lax.broadcasted_iota(i32, (shards * 8, LANES), 0)
    down = lax.broadcasted_iota(i32, (LANES, LANES), 0)
    for b in range(lines):
        here = slice(b * LANES, (b + 1) * LANES)
        s.ha[:, here] = jnp.where(
            jnp.broadcast_to(high[b : b + 1, :], (shards * 8, LANES)) == tile_of, 1.0, 0.0
        ).astype(bf16)
        s.hb[:, here] = jnp.where(
            jnp.broadcast_to(low[b : b + 1, :], (LANES, LANES)) == down, 1.0, 0.0
        ).astype(bf16)
    s.hist[...] = lax.dot_general(s.ha[...], s.hb[...], (((1,), (1,)), ((), ())), preferred_element_type=f32)
    tallied = {}
    for p in range(1, shards):
        t = lax.rem(me + p, shards)
        tallied[p] = started(
            s.hist.at[pl.ds(pl.multiple_of(t * 8, 8), 8)], s.hs.at[p], s.sh.at[p - 1], s.rh.at[p - 1], peers[p]
        )
    s.hs[0] = s.hist[pl.ds(pl.multiple_of(me * 8, 8), 8), :]

    loads[7].wait()
    loads[8].wait()

    def lay(e):
        here = pl.ds(e * SPAN, SPAN)
        for h in range(parts):
            hi, lo = pieces(s.inbox[h, here, :])
            s.dp[here, 2 * h * LANES : (2 * h + 1) * LANES] = hi
            s.dp[here, (2 * h + 1) * LANES : (2 * h + 2) * LANES] = lo
        s.dp[here, 2 * parts * LANES :] = jnp.ones((SPAN, LANES), bf16)

    each(joined // SPAN, lay)

    def move(e):
        first = (jnp.int32(e) * height).astype(f32)
        one_hot(lambda b: s.lab[b : b + 1, :] - first, across, s.oh1, height)
        s.sums[...] = jnp.dot(s.oh1[...], s.dp[...], preferred_element_type=f32)
        for sub in range(height // LANES):
            b = e * (height // LANES) + sub
            here = pl.ds(pl.multiple_of(b * LANES, LANES), LANES)
            local = slice(sub * LANES, (sub + 1) * LANES)
            m = s.sums[local, 2 * parts * LANES :]
            n = to_column(s.counts[pl.ds(b, 1), :], same) + m
            r = 1.0 / n
            for h in range(parts):
                total = s.sums[local, 2 * h * LANES : (2 * h + 1) * LANES] + s.sums[
                    local, (2 * h + 1) * LANES : (2 * h + 2) * LANES
                ]
                old = s.cent[here, h * LANES : (h + 1) * LANES]
                moved[here, h * LANES : (h + 1) * LANES] = old + (total - m * old) * r
            news[pl.ds(b, 1), :] = to_row(n, same)

    each(count // height, move)

    for h in range(1, parts):
        forward(h)
        region("own", base(h))
        ahead(h, ("own",))
        combine(h, "own")

    tally = s.hs[0]
    for p in range(1, shards):
        tallied[p].wait_recv()
        tally = tally + s.hs[p]
    members = tally[:tall, :block]
    upnews[...] = s.weights[...] + members
    square_block = square(block)

    def finish(h):
        base_i = h * chips
        for dy in range(1, ys):
            a1(dy, 0, h).wait_recv()
        for dx in range(1, xs):
            b1(0, dx, h).wait_recv()
        for dx in range(1, xs):
            a2(dx, h).wait_recv()
        for dy in range(1, ys):
            b2(dy, h).wait_recv()
        total = s.chip[base_i, :half]
        for dy in range(1, ys):
            total = total + s.a1[h * na + (dy - 1) * xs]
        for dx in range(1, xs):
            total = total + s.a2[h * (xs - 1) + dx - 1]
        s.fin[:half] = total
        total = s.chip[base_i, half:]
        for dx in range(1, xs):
            total = total + s.b1[h * nb + (dx - 1) * ys]
        for dy in range(1, ys):
            total = total + s.b2[h * (ys - 1) + dy - 1]
        s.fin[half:] = total
        for line in range(tall):
            here = slice(line * block, (line + 1) * block)
            m = to_column(members[line : line + 1, :], square_block)
            n = to_column(s.weights[line : line + 1, :], square_block) + m
            prev = s.upper[here, h * LANES : (h + 1) * LANES]
            newup[here, h * LANES : (h + 1) * LANES] = prev + (s.fin[here, :] - m * prev) / n

    for h in range(parts):
        finish(h)

    for copy in list(asked.values()) + list(sent.values()) + list(moves.values()):
        copy.wait_send()
    for copy in list(told.values()) + list(tallied.values()) + [linked]:
        copy.wait_send()
    each(parts * chips, lambda i: pair(jnp.int32(i), 0).wait_send())
    for h in range(parts):
        give(h).wait_send()
        for name in ("diag", "dy"):
            region(name, lambda dy, dx: a1(dy, dx, h).wait_send())
        for name in ("diag", "dx"):
            region(name, lambda dy, dx: b1(dy, dx, h).wait_send())
        for dx in range(1, xs):
            a2(dx, h).wait_send()
        for dy in range(1, ys):
            b2(dy, h).wait_send()


def emit_kernel(moved_v, news_v, up_v, upnews_v, moved, news, up, upnews, sems):
    copies = [
        pltpu.make_async_copy(src, dst, sems.at[i])
        for i, (src, dst) in enumerate(((moved_v, moved), (up_v, up), (news_v, news), (upnews_v, upnews)))
    ]
    for copy in copies:
        copy.start()
    for copy in copies:
        copy.wait()


def body(
    rows_data, owner_rows, slot_rows, centroids, counts, owner_cent, slot_cent, upper, upper_counts
):
    zs, ys, xs = lax.axis_size("rows"), lax.axis_size("cx"), lax.axis_size("cy") // CORES
    chips = ys * xs
    shards = chips * CORES
    batch, features = rows_data.shape
    count, width = centroids.shape
    parts = width // LANES
    slots = upper.shape[0]
    half = slots // 2
    block = min(LANES, slots)
    capacity = -(-(2 * batch // shards) // 8) * 8
    spots = shards * capacity
    across = zs * spots // LANES
    joined = across * LANES
    tall = -(-zs // 8) * 8
    padded = -(-across // 8) * 8
    band = min(joined, 512)
    height = min(count, 512)
    na, nb = (ys - 1) * xs, (xs - 1) * ys

    vm = pl.BlockSpec(memory_space=pltpu.VMEM)
    hbm = pl.BlockSpec(memory_space=pl.ANY)
    V = pltpu.VMEM
    dma = lambda n: pltpu.SemaphoreType.DMA((n,))
    scratch = dict(
        oc=V((1, count), i32), sc=V((count // LANES, LANES), i32), cent=V((count, width), f32),
        owner=V((1, batch), i32), slot=V((1, batch), i32), rows=V((batch, features), f32),
        counts=V((count // LANES, LANES), f32), upper=V((slots, width), f32),
        weights=V((slots // block, block), f32),
        own=V((count // LANES, LANES), i32), uid=V((count // LANES, LANES), f32),
        cp=V((parts, count, 2 * LANES), bf16), oh=V((2, slots, count), bf16),
        outp=V((parts * chips, slots, LANES), f32), pair=V((parts * chips, slots, LANES), f32),
        base=V((parts * chips, slots, LANES), f32), chip=V((parts * chips, slots, LANES), f32),
        info=V((8, LANES), i32), mine=V((zs, 8, LANES), i32),
        slabs=V((parts * zs, batch, LANES), f32), pick=V((zs, spots, LANES), bf16),
        packed=V((parts * zs, spots, LANES), f32), inbox=V((parts, joined, LANES), f32),
        tags=V((tall, spots), i32), heard=V((shards, tall, spots), i32),
        ha=V((shards * 8, count), bf16), hb=V((LANES, count), bf16), hist=V((shards * 8, LANES), f32),
        hs=V((shards, 8, LANES), f32), lab=V((padded, LANES), f32), urow=V((padded, LANES), f32),
        prow=V((padded, LANES), f32), ot=V((band, count), bf16), tab=V((LANES, 5 * LANES), bf16), share=V((joined, LANES), f32),
        near=V((parts, joined, LANES), f32), dl=V((parts, joined, LANES), f32),
        pd=V((parts, joined, LANES), f32), dd=V((parts, 2 * joined, 2 * LANES), bf16),
        oh3=V((chips if parts > 1 else 1, slots, 2 * joined), bf16),
        a1=V((parts * na, half, LANES), f32), b1=V((parts * nb, half, LANES), f32),
        a2=V((parts * (xs - 1), half, LANES), f32), b2=V((parts * (ys - 1), half, LANES), f32),
        relay_a=V((parts * (xs - 1), half, LANES), f32), relay_b=V((parts * (ys - 1), half, LANES), f32),
        dp=V((joined, (2 * parts + 1) * LANES), bf16), oh1=V((height, joined), bf16),
        sums=V((height, (2 * parts + 1) * LANES), f32), fin=V((slots, LANES), f32),
        ld=dma(9), si=dma(zs - 1), ri=dma(zs - 1), ss=dma(parts * (zs - 1)), rs=dma(parts * (zs - 1)),
        sp=dma((shards - 1) * zs * parts), rp=dma((shards - 1) * zs * parts),
        st=dma(shards - 1), rt=dma(shards - 1), sh=dma(shards - 1), rh=dma(shards - 1),
        sb=dma(parts * chips), rb=dma(parts * chips), su=dma(1), ru=dma(1), sd=dma(parts), rd=dma(parts),
        sa1=dma(parts * na), ra1=dma(parts * na), sb1=dma(parts * nb), rb1=dma(parts * nb),
        sa2=dma(parts * (xs - 1)), ra2=dma(parts * (xs - 1)), sb2=dma(parts * (ys - 1)), rb2=dma(parts * (ys - 1)),
    )
    outs = (
        jax.ShapeDtypeStruct((count, width), f32),
        jax.ShapeDtypeStruct((count // LANES, LANES), f32),
        jax.ShapeDtypeStruct((slots, width), f32),
        jax.ShapeDtypeStruct((slots // block, block), f32),
    )
    made = pl.pallas_call(
        functools.partial(fused_kernel, tuple(scratch), (zs, ys, xs, capacity, height)),
        out_shape=outs,
        in_specs=[pl.BlockSpec(memory_space=pltpu.HBM)] * 9,
        out_specs=(vm,) * 4,
        scratch_shapes=list(scratch.values()),
        compiler_params=pltpu.CompilerParams(
            collective_id=1, has_side_effects=True, vmem_limit_bytes=44 * 1024 * 1024
        ),
        name="update",
    )(*[pltpu.with_memory_space_constraint(a, pltpu.HBM) for a in (
        rows_data, owner_rows.reshape(1, batch), slot_rows.reshape(1, batch), centroids,
        counts.reshape(-1, LANES), owner_cent.reshape(1, count), slot_cent.reshape(-1, LANES),
        upper, upper_counts.reshape(-1, block),
    )])
    moved, news, new_upper, upnews = pl.pallas_call(
        emit_kernel,
        out_shape=outs,
        in_specs=[vm] * 4,
        out_specs=(hbm,) * 4,
        scratch_shapes=[dma(4)],
        compiler_params=pltpu.CompilerParams(vmem_limit_bytes=4 * 1024 * 1024),
        name="emit",
    )(*made)
    return moved, news.reshape(-1), new_upper, upnews.reshape(-1)


def solution(mesh):
    placed = (
        P(("rows", "cx", "cy"), None),
        P(("rows", "cx", "cy"), None),
        P(("rows", "cx", "cy")),
        P(("cx", "cy"), "rows"),
        P(("cx", "cy")),
        P(("cx", "cy"), None),
        P(("cx", "cy")),
        P(("cx", "cy"), "rows"),
        P(("cx", "cy")),
    )
    return jax.shard_map(
        body,
        mesh=mesh,
        in_specs=placed,
        out_specs=(
            P(("cx", "cy"), "rows"),
            P(("cx", "cy")),
            P(("cx", "cy"), "rows"),
            P(("cx", "cy")),
        ),
        check_vma=False,
    )
```

```python
import functools
import types

import jax
import jax.numpy as jnp
from jax import lax
from jax.experimental import pallas as pl
from jax.experimental.pallas import tpu as pltpu
from jax.sharding import PartitionSpec as P

MESH = pl.DeviceIdType.MESH
LANES = 128
CORES = 2
SPAN = 256
bf16, f32, i32 = jnp.bfloat16, jnp.float32, jnp.int32


def pieces(x):
    first = x.astype(bf16)
    return first, (x - first.astype(f32)).astype(bf16)


def halves(x):
    return x[:, :LANES] + x[:, LANES : 2 * LANES]


def square(size):
    up = lax.broadcasted_iota(i32, (size, size), 0)
    return up == lax.broadcasted_iota(i32, (size, size), 1)


def to_column(row, same):
    size = row.shape[1]
    return jnp.sum(jnp.where(same, jnp.broadcast_to(row, (size, size)), 0.0), axis=1, keepdims=True)


def to_row(column, same):
    return jnp.sum(jnp.where(same, jnp.broadcast_to(column, same.shape), 0.0), axis=0, keepdims=True)


def each(count, step):
    if count == 1:
        step(0)
    elif count > 1:
        lax.fori_loop(0, count, lambda e, c: (step(e), c)[1], 0)


def one_hot(row_of, lines, out, height):
    span = min(SPAN, height)
    spots = lax.broadcasted_iota(i32, (span, LANES), 0).astype(f32).astype(bf16)
    one, zero = jnp.ones((span, LANES), bf16), jnp.zeros((span, LANES), bf16)
    for q in range(height // span):
        for b in range(lines):
            row = jnp.broadcast_to(row_of(b) - float(q * span), (16, LANES)).astype(bf16)
            row = jnp.concatenate([row] * (span // 16), axis=0)
            out[q * span : (q + 1) * span, b * LANES : (b + 1) * LANES] = jnp.where(row == spots, one, zero)


def fused_kernel(
    names, sizes, rows_h, owner_h, slot_h, cent_h, counts_h, oc_h, sc_h, upper_h, weights_h,
    moved, news, newup, upnews, *scratch,
):
    s = types.SimpleNamespace(**dict(zip(names, scratch)))
    zs, ys, xs, capacity, height = sizes
    chips, cys = ys * xs, xs * CORES
    shards = chips * CORES
    batch = rows_h.shape[0]
    count, width = cent_h.shape
    parts = width // LANES
    lines = count // LANES
    slots = upper_h.shape[0]
    half = slots // 2
    tall, block = weights_h.shape
    spots = shards * capacity
    per = LANES // capacity
    across = zs * spots // LANES
    joined = across * LANES

    z, y, cy = lax.axis_index("rows"), lax.axis_index("cx"), lax.axis_index("cy")
    x, core = lax.div(cy, CORES), lax.rem(cy, CORES)
    me = y * cys + cy
    other = {"cx": y, "cy": x * CORES + 1 - core}

    def mate(d):
        if zs & (zs - 1):
            return lax.rem(z + d, zs)
        at = z
        bit = 1
        while bit <= d:
            if d & bit:
                at = at + bit * (1 - 2 * lax.rem(lax.div(z, bit), 2))
            bit *= 2
        return at

    mates = {d: {"rows": mate(d)} for d in range(1, zs)}
    peers = {}
    for p in range(1, shards):
        t = lax.rem(me + p, shards)
        peers[p] = {"cx": lax.div(t, cys), "cy": lax.rem(t, cys)}

    barrier = pltpu.get_barrier_semaphore()
    for peer in list(mates.values()) + list(peers.values()):
        pl.semaphore_signal(barrier, inc=1, device_id=peer, device_id_type=MESH)

    loads = [
        pltpu.make_async_copy(src, dst, s.ld.at[i])
        for i, (src, dst) in enumerate([
            (owner_h, s.owner), (slot_h, s.slot), (rows_h, s.rows), (oc_h, s.oc), (sc_h, s.sc),
            (cent_h, s.cent), (counts_h, s.counts), (upper_h, s.upper), (weights_h, s.weights),
        ])
    ]
    for copy in loads:
        copy.start()

    def remote(src, dst, send, recv, peer):
        return pltpu.make_async_remote_copy(
            src_ref=src, dst_ref=dst, send_sem=send, recv_sem=recv, device_id=peer, device_id_type=MESH
        )

    def started(*args):
        copy = remote(*args)
        copy.start()
        return copy

    same = square(LANES)
    lane = lax.broadcasted_iota(i32, (LANES, LANES), 1)

    regions = {
        "diag": ((ys - 1) * (xs - 1), lambda e: (1 + lax.div(e, xs - 1), 1 + lax.rem(e, xs - 1))),
        "dy": (ys - 1, lambda e: (1 + e, 0)),
        "dx": (xs - 1, lambda e: (0, 1 + e)),
        "own": (1, lambda e: (0, 0)),
    }

    def region(name, step):
        number, where = regions[name]

        def run(e):
            if isinstance(e, int):
                e = jnp.int32(e)
            step(*where(e))

        each(number, run)

    def shard_at(dy, dx, side):
        return (lax.rem(y + dy, ys) * xs + lax.rem(x + dx, xs)) * CORES + side

    loads[0].wait()
    loads[1].wait()
    loads[2].wait()
    s.info[...] = jnp.full_like(s.info, -1)
    s.info[0:1, :batch] = s.owner[...]
    s.info[1:2, :batch] = s.slot[...]
    s.tags[...] = jnp.full_like(s.tags, count)
    pl.semaphore_wait(barrier, zs - 1 + shards - 1)

    targets = []
    low_end, high_end = jnp.int32(0), jnp.int32(zs - 1)
    for _ in range(1, zs):
        under, over = z - low_end, high_end - z
        take = (under > over) | ((under == over) & (2 * z < zs))
        targets.append(jnp.where(take, low_end, high_end))
        low_end = low_end + jnp.where(take, 1, 0)
        high_end = high_end - jnp.where(take, 0, 1)

    def place_of(t):
        if zs & (zs - 1):
            return lax.rem(t - z + zs, zs)
        total, bit = 0, 1
        while bit < zs:
            total = total + bit * lax.rem(lax.div(z, bit) + lax.div(t, bit), 2)
            bit *= 2
        return total

    def ask(d, t):
        return remote(s.info, s.mine.at[d], s.si.at[d - 1], s.ri.at[d - 1], {"rows": t})

    def slab(d, t, h):
        here = pl.ds(pl.multiple_of(t * width + h * LANES, LANES), LANES)
        i = h * (zs - 1) + d - 1
        return remote(s.rows.at[:, here], s.slabs.at[h * zs + d], s.ss.at[i], s.rs.at[i], {"rows": t})

    asked = {d: ask(d, mates[d]["rows"]) for d in range(1, zs)}
    sent = {(h, d): slab(d, mates[d]["rows"], h) for h in range(parts) for d in range(1, zs)}
    for t in targets:
        ask(place_of(t), t).start()

    def scatter(h):
        for t in targets:
            slab(place_of(t), t, h).start()

    scatter(0)
    s.mine[0] = s.info[...]
    for h in range(parts):
        s.slabs[h * zs] = s.rows[:, pl.ds(pl.multiple_of(z * width + h * LANES, LANES), LANES)]

    before = jnp.where(lax.broadcasted_iota(i32, (LANES, LANES), 0) < lane, 1.0, 0.0).astype(bf16)
    shard_of = lax.broadcasted_iota(i32, (shards, LANES), 0)
    spot_of = lax.broadcasted_iota(i32, (spots, LANES), 0)
    line_of = lax.broadcasted_iota(i32, (8, LANES), 0)

    def place(d):
        owner, slot = s.mine[d, 0:1, :], s.mine[d, 1:2, :]
        named = jnp.where(jnp.broadcast_to(owner, (shards, LANES)) == shard_of, 1.0, 0.0)
        earlier = jnp.dot(named.astype(bf16), before, preferred_element_type=f32)
        position = jnp.sum(named * earlier, axis=0, keepdims=True).astype(i32)
        target = jnp.where(owner >= 0, owner * capacity + position, -1)
        pick = jnp.where(jnp.broadcast_to(target, (spots, LANES)) == spot_of, 1.0, 0.0).astype(bf16)
        s.pick[d] = pick
        high = jnp.broadcast_to(lax.shift_right_arithmetic(slot, 7), (8, LANES))
        low = jnp.broadcast_to(slot & 127, (8, LANES))
        code = jnp.where(line_of == 0, high, jnp.where(line_of == 1, low, 1)).astype(f32).astype(bf16)
        found = lax.dot_general(code, pick, (((1,), (1,)), ((), ())), preferred_element_type=f32)
        tag = (found[0:1] * 128.0 + found[1:2]).astype(i32)
        s.tags[d : d + 1, :] = jnp.where(found[2:3] > 0.5, tag, count)

    def spot(p, d):
        return ((p // per) * zs + d) * LANES + (p % per) * capacity

    moves = {}

    def pack(d, h):
        slab = s.slabs[h * zs + d]
        hi, mid = pieces(slab)
        low = (slab - hi.astype(f32) - mid.astype(f32)).astype(bf16)
        three = jnp.concatenate([hi, mid, low], axis=1)
        total = jnp.dot(s.pick[d, :, :batch], three, preferred_element_type=f32)
        total = (total[:, 2 * LANES :] + total[:, LANES : 2 * LANES]) + total[:, :LANES]
        s.packed[h * zs + d] = total

    def post(d, h):
        for p in range(1, shards):
            t = lax.rem(me + p, shards)
            i = ((p - 1) * zs + d) * parts + h
            moves[p, d, h] = started(
                s.packed.at[h * zs + d, pl.ds(pl.multiple_of(t * capacity, 8), capacity)],
                s.inbox.at[h, pl.ds(spot(p, d), capacity)], s.sp.at[i], s.rp.at[i], peers[p],
            )

    def keep(d, h):
        s.inbox[h, spot(0, d) : spot(0, d) + capacity, :] = s.packed[
            h * zs + d, pl.ds(pl.multiple_of(me * capacity, 8), capacity), :
        ]

    place(0)
    for h in range(parts):
        pack(0, h)
    for h in range(parts):
        post(0, h)
        keep(0, h)

    loads[3].wait()
    loads[4].wait()
    for b in range(lines):
        s.own[b : b + 1, :] = s.oc[0:1, b * LANES : (b + 1) * LANES]
    s.uid[...] = (s.own[...] * slots + s.sc[...]).astype(f32)
    loads[5].wait()

    def split(b, c):
        here = pl.ds(pl.multiple_of(b * SPAN, SPAN), SPAN)
        for h in range(parts):
            hi, lo = pieces(s.cent[here, h * LANES : (h + 1) * LANES])
            s.cp[h, here, :LANES] = hi
            s.cp[h, here, LANES:] = lo
        return c

    lax.fori_loop(0, count // SPAN, split, 0)
    loads[6].wait()
    s.tab[...] = jnp.zeros_like(s.tab)
    near_c, mid_c = pieces(s.counts[...])
    far_c = (s.counts[...] - near_c.astype(f32) - mid_c.astype(f32)).astype(bf16)
    for i, part in enumerate((near_c, mid_c, far_c) + pieces(s.uid[...])):
        s.tab[:lines, i * LANES : (i + 1) * LANES] = part

    def pair(k, h):
        i = h * chips + k
        return remote(s.outp.at[i], s.pair.at[i], s.sb.at[i], s.rb.at[i], other)

    def base(h):
        def step(dy, dx):
            k = dy * xs + dx
            i = h * chips + k
            for mine_too, side in ((0, 1 - core), (1, core)):
                first = (shard_at(dy, dx, side) * slots).astype(f32)
                one_hot(lambda b: s.uid[b : b + 1, :] - first, lines, s.oh.at[mine_too], slots)
                total = halves(jnp.dot(s.oh[mine_too], s.cp[h], preferred_element_type=f32))
                if mine_too:
                    s.base[i] = total
                else:
                    s.outp[i] = total
            pair(k, h).start()

        return step

    region("diag", base(0))
    region("dy", base(0))
    for h in range(1, parts):
        scatter(h)

    for d in range(1, zs):
        asked[d].wait_recv()
    for d in range(1, zs):
        place(d)
    told = {p: started(s.tags, s.heard.at[p], s.st.at[p - 1], s.rt.at[p - 1], peers[p]) for p in range(1, shards)}
    s.heard[0] = s.tags[...]

    def relay(h):
        for d in range(1, zs):
            sent[h, d].wait_recv()
        for d in range(1, zs):
            pack(d, h)
        for d in range(1, zs):
            post(d, h)

    for d in range(1, zs):
        sent[0, d].wait_recv()
        pack(d, 0)
        post(d, 0)
    for d in range(1, zs):
        keep(d, 0)
    region("dx", base(0))

    for p in range(1, shards):
        told[p].wait_recv()
    few = lax.broadcasted_iota(i32, (s.tags.shape[0], LANES), 1)
    s.lab[...] = jnp.full_like(s.lab, count)
    for g in range(shards // per):
        both = jnp.full(few.shape, count, i32)
        for j in range(per):
            turn = lax.rem((j + shards - me) * capacity, spots)
            turned = pltpu.roll(s.heard[g * per + j], turn, 1)[:, :LANES]
            both = jnp.where((few >= j * capacity) & (few < (j + 1) * capacity), turned, both)
        s.lab[g * zs : (g + 1) * zs, :] = both[:zs].astype(f32)

    band = s.ot.shape[0]

    def fetch(jb, h):
        here = pl.ds(pl.multiple_of(jb * band, band), band)
        s.near[h, here, :] = halves(jnp.dot(s.ot[...], s.cp[h], preferred_element_type=f32))

    across_f = lane.astype(f32)
    across_h = across_f.astype(bf16)
    unit, none = jnp.ones((LANES, LANES), bf16), jnp.zeros((LANES, LANES), bf16)

    def gather(jb):
        for rr in range(band // LANES):
            r = jb * (band // LANES) + rr
            here = pl.ds(pl.multiple_of(r * LANES, LANES), LANES)
            row = s.lab[pl.ds(r, 1), :]
            column = to_column(row, same)
            top = jnp.floor(column * (1.0 / LANES))
            label = jnp.broadcast_to(column, (LANES, LANES))
            major = jnp.broadcast_to(top, (LANES, LANES))
            minor = jnp.broadcast_to(column - top * float(LANES), (LANES, LANES))

            def alike(q, total):
                return total + jnp.where(label == s.lab[pl.ds(q, 1), :], 1.0, 0.0)

            total = jnp.zeros((LANES, LANES), f32)
            if across <= 8:
                for q in range(across):
                    total = alike(q, total)
            else:
                total = lax.fori_loop(0, across, alike, total)
            line_at = jnp.where(across_f == major, 1.0, 0.0).astype(bf16)
            found = jnp.dot(line_at, s.tab[...], preferred_element_type=f32)
            had = (found[:, :LANES] + found[:, LANES : 2 * LANES]) + found[:, 2 * LANES : 3 * LANES]
            named = found[:, 3 * LANES : 4 * LANES] + found[:, 4 * LANES :]
            hit = across_f == minor
            n = jnp.sum(jnp.where(hit, had, 0.0) + total, axis=1, keepdims=True)
            s.share[here, :] = jnp.broadcast_to(1.0 / n, (LANES, LANES))
            target = to_row(jnp.sum(jnp.where(hit, named, 0.0), axis=1, keepdims=True), same)
            s.urow[pl.ds(r, 1), :] = jnp.where(row < float(count), target, -1.0)
            spread = jnp.where(minor.astype(bf16) == across_h, unit, none)
            major_h = major.astype(bf16)
            for b in range(lines):
                s.ot[rr * LANES : (rr + 1) * LANES, b * LANES : (b + 1) * LANES] = jnp.where(
                    major_h == jnp.full((LANES, LANES), float(b), bf16), spread, none
                )
        for h in range(parts if joined > band else 1):
            fetch(jb, h)

    s.urow[...] = jnp.full_like(s.urow, -1.0)
    each(joined // band, gather)
    linked = started(s.urow, s.prow, s.su.at[0], s.ru.at[0], other)
    ready = parts > 1

    def aim(rows, begin):
        def step(dy, dx):
            k = (dy * xs + dx) if ready else 0
            first = (shard_at(dy, dx, core) * slots).astype(f32)
            one_hot(
                lambda b: rows[b : b + 1, :] - first, across, s.oh3.at[k, :, pl.ds(begin, joined)], slots
            )

        return step


    def give(h):
        return remote(s.dl.at[h], s.pd.at[h], s.sd.at[h], s.rd.at[h], other)

    def change(h):
        for p in range(1, shards):
            for d in range(zs):
                moves[p, d, h].wait_recv()

        def step(e):
            here = pl.ds(e * SPAN, SPAN)
            s.dl[h, here, :] = (s.inbox[h, here, :] - s.near[h, here, :]) * s.share[here, :]

        each(joined // SPAN, step)
        give(h).start()

        def cut(e):
            here = pl.ds(e * SPAN, SPAN)
            hi, lo = pieces(s.dl[h, here, :])
            s.dd[h, here, :LANES] = hi
            s.dd[h, here, LANES:] = lo

        each(joined // SPAN, cut)

    def accept(h):
        give(h).wait_recv()

        def cut(e):
            here = pl.ds(e * SPAN, SPAN)
            there = pl.ds(e * SPAN + joined, SPAN)
            hi, lo = pieces(s.pd[h, here, :])
            s.dd[h, there, :LANES] = hi
            s.dd[h, there, LANES:] = lo

        each(joined // SPAN, cut)

    def at(dy, dx):
        return lax.rem(y + dy, ys), lax.rem(x + dx, xs)

    na, nb = (ys - 1) * xs, (xs - 1) * ys

    def a1(dy, dx, h):
        i = h * na + (dy - 1) * xs + dx
        return remote(
            s.chip.at[h * chips + dy * xs + dx, pl.ds(0, half)], s.a1.at[i], s.sa1.at[i], s.ra1.at[i],
            {"cx": lax.rem(y + dy, ys), "cy": cy},
        )

    def b1(dy, dx, h):
        i = h * nb + (dx - 1) * ys + dy
        return remote(
            s.chip.at[h * chips + dy * xs + dx, pl.ds(half, half)], s.b1.at[i], s.sb1.at[i], s.rb1.at[i],
            {"cx": y, "cy": lax.rem(x + dx, xs) * CORES + core},
        )

    def a2(dx, h):
        i = h * (xs - 1) + dx - 1
        return remote(
            s.relay_a.at[i], s.a2.at[i], s.sa2.at[i], s.ra2.at[i],
            {"cx": y, "cy": lax.rem(x + dx, xs) * CORES + core},
        )

    def b2(dy, h):
        i = h * (ys - 1) + dy - 1
        return remote(
            s.relay_b.at[i], s.b2.at[i], s.sb2.at[i], s.rb2.at[i],
            {"cx": lax.rem(y + dy, ys), "cy": cy},
        )

    def prepare(h):
        def step(dy, dx):
            k = dy * xs + dx
            i = h * chips + k
            o = k if ready else 0
            if not ready:
                aim(s.urow, 0)(dy, dx)
                aim(s.prow, joined)(dy, dx)
            pair(k, h).wait_recv()
            total = halves(jnp.dot(s.oh3[o, :, :joined], s.dd[h, :joined, :], preferred_element_type=f32))
            s.chip[i] = total + (s.base[i] + s.pair[i])

        return step

    def combine(h, name):
        def step(dy, dx):
            k = dy * xs + dx
            i = h * chips + k
            o = k if ready else 0
            if not ready:
                prepare(h)(dy, dx)
            total = halves(jnp.dot(s.oh3[o, :, joined:], s.dd[h, joined:, :], preferred_element_type=f32))
            s.chip[i] = s.chip[i] + total
            if name in ("diag", "dy"):
                a1(dy, dx, h).start()
            if name in ("diag", "dx"):
                b1(dy, dx, h).start()

        region(name, step)

    def ahead(h, names):
        if ready:
            for name in names:
                region(name, prepare(h))

    def forward(h):
        for dx in range(1, xs):
            i = h * chips + dx
            total = s.chip[i, :half]
            for dy in range(1, ys):
                a1(dy, dx, h).wait_recv()
                total = total + s.a1[h * na + (dy - 1) * xs + dx]
            s.relay_a[h * (xs - 1) + dx - 1] = total
            a2(dx, h).start()
        for dy in range(1, ys):
            i = h * chips + dy * xs
            total = s.chip[i, half:]
            for dx in range(1, xs):
                b1(dy, dx, h).wait_recv()
                total = total + s.b1[h * nb + (dx - 1) * ys + dy]
            s.relay_b[h * (ys - 1) + dy - 1] = total
            b2(dy, h).start()

    change(0)
    if ready:
        region("diag", aim(s.urow, 0))
    linked.wait_recv()
    if ready:
        region("diag", aim(s.prow, joined))
    ahead(0, ("diag",))
    for h in range(1, parts):
        relay(h)
        for d in range(1, zs):
            keep(d, h)
    accept(0)
    combine(0, "diag")
    if ready:
        for name in ("dy", "dx"):
            region(name, aim(s.urow, 0))
            region(name, aim(s.prow, joined))
    ahead(0, ("dy", "dx"))
    combine(0, "dy")
    combine(0, "dx")
    for h in range(1, parts):
        if joined <= band:
            fetch(0, h)
        region("diag", base(h))
        region("dy", base(h))
        change(h)
        if h == 1:
            forward(0)
        region("dx", base(h))
        ahead(h, ("diag", "dy", "dx"))
        accept(h)
        for name in ("diag", "dy", "dx"):
            combine(h, name)
    if parts == 1:
        forward(0)
    region("own", base(0))
    if ready:
        region("own", aim(s.urow, 0))
        region("own", aim(s.prow, joined))
    ahead(0, ("own",))
    combine(0, "own")

    high = s.own[...] * 8 + lax.div(s.sc[...], block)
    low = lax.rem(s.sc[...], block)
    tile_of = lax.broadcasted_iota(i32, (shards * 8, LANES), 0)
    down = lax.broadcasted_iota(i32, (LANES, LANES), 0)
    for b in range(lines):
        here = slice(b * LANES, (b + 1) * LANES)
        s.ha[:, here] = jnp.where(
            jnp.broadcast_to(high[b : b + 1, :], (shards * 8, LANES)) == tile_of, 1.0, 0.0
        ).astype(bf16)
        s.hb[:, here] = jnp.where(
            jnp.broadcast_to(low[b : b + 1, :], (LANES, LANES)) == down, 1.0, 0.0
        ).astype(bf16)
    s.hist[...] = lax.dot_general(s.ha[...], s.hb[...], (((1,), (1,)), ((), ())), preferred_element_type=f32)
    tallied = {}
    for p in range(1, shards):
        t = lax.rem(me + p, shards)
        tallied[p] = started(
            s.hist.at[pl.ds(pl.multiple_of(t * 8, 8), 8)], s.hs.at[p], s.sh.at[p - 1], s.rh.at[p - 1], peers[p]
        )
    s.hs[0] = s.hist[pl.ds(pl.multiple_of(me * 8, 8), 8), :]

    loads[7].wait()
    loads[8].wait()

    def lay(e):
        here = pl.ds(e * SPAN, SPAN)
        for h in range(parts):
            hi, lo = pieces(s.inbox[h, here, :])
            s.dp[here, 2 * h * LANES : (2 * h + 1) * LANES] = hi
            s.dp[here, (2 * h + 1) * LANES : (2 * h + 2) * LANES] = lo
        s.dp[here, 2 * parts * LANES :] = jnp.ones((SPAN, LANES), bf16)

    each(joined // SPAN, lay)

    def move(e):
        first = (jnp.int32(e) * height).astype(f32)
        one_hot(lambda b: s.lab[b : b + 1, :] - first, across, s.oh1, height)
        s.sums[...] = jnp.dot(s.oh1[...], s.dp[...], preferred_element_type=f32)
        for sub in range(height // LANES):
            b = e * (height // LANES) + sub
            here = pl.ds(pl.multiple_of(b * LANES, LANES), LANES)
            local = slice(sub * LANES, (sub + 1) * LANES)
            m = s.sums[local, 2 * parts * LANES :]
            n = to_column(s.counts[pl.ds(b, 1), :], same) + m
            r = 1.0 / n
            for h in range(parts):
                total = s.sums[local, 2 * h * LANES : (2 * h + 1) * LANES] + s.sums[
                    local, (2 * h + 1) * LANES : (2 * h + 2) * LANES
                ]
                old = s.cent[here, h * LANES : (h + 1) * LANES]
                moved[here, h * LANES : (h + 1) * LANES] = old + (total - m * old) * r
            news[pl.ds(b, 1), :] = to_row(n, same)

    each(count // height, move)

    for h in range(1, parts):
        forward(h)
        region("own", base(h))
        ahead(h, ("own",))
        combine(h, "own")

    tally = s.hs[0]
    for p in range(1, shards):
        tallied[p].wait_recv()
        tally = tally + s.hs[p]
    members = tally[:tall, :block]
    upnews[...] = s.weights[...] + members
    square_block = square(block)
    for line in range(tall):
        here = slice(line * block, (line + 1) * block)
        m = to_column(members[line : line + 1, :], square_block)
        n = to_column(s.weights[line : line + 1, :], square_block) + m
        s.mcol[here, :] = jnp.broadcast_to(m, (block, LANES))
        s.ncol[here, :] = jnp.broadcast_to(1.0 / n, (block, LANES))

    def finish(h):
        base_i = h * chips
        for dy in range(1, ys):
            a1(dy, 0, h).wait_recv()
        for dx in range(1, xs):
            b1(0, dx, h).wait_recv()
        for dx in range(1, xs):
            a2(dx, h).wait_recv()
        for dy in range(1, ys):
            b2(dy, h).wait_recv()
        total = s.chip[base_i, :half]
        for dy in range(1, ys):
            total = total + s.a1[h * na + (dy - 1) * xs]
        for dx in range(1, xs):
            total = total + s.a2[h * (xs - 1) + dx - 1]
        s.fin[:half] = total
        total = s.chip[base_i, half:]
        for dx in range(1, xs):
            total = total + s.b1[h * nb + (dx - 1) * ys]
        for dy in range(1, ys):
            total = total + s.b2[h * (ys - 1) + dy - 1]
        s.fin[half:] = total
        prev = s.upper[:, h * LANES : (h + 1) * LANES]
        newup[:, h * LANES : (h + 1) * LANES] = prev + (s.fin[...] - s.mcol[...] * prev) * s.ncol[...]

    for h in range(parts):
        finish(h)

    for copy in list(asked.values()) + list(sent.values()) + list(moves.values()):
        copy.wait_send()
    for copy in list(told.values()) + list(tallied.values()) + [linked]:
        copy.wait_send()
    each(parts * chips, lambda i: pair(jnp.int32(i), 0).wait_send())
    for h in range(parts):
        give(h).wait_send()
        for name in ("diag", "dy"):
            region(name, lambda dy, dx: a1(dy, dx, h).wait_send())
        for name in ("diag", "dx"):
            region(name, lambda dy, dx: b1(dy, dx, h).wait_send())
        for dx in range(1, xs):
            a2(dx, h).wait_send()
        for dy in range(1, ys):
            b2(dy, h).wait_send()


def emit_kernel(moved_v, news_v, up_v, upnews_v, moved, news, up, upnews, sems):
    copies = [
        pltpu.make_async_copy(src, dst, sems.at[i])
        for i, (src, dst) in enumerate(((moved_v, moved), (up_v, up), (news_v, news), (upnews_v, upnews)))
    ]
    for copy in copies:
        copy.start()
    for copy in copies:
        copy.wait()


def body(
    rows_data, owner_rows, slot_rows, centroids, counts, owner_cent, slot_cent, upper, upper_counts
):
    zs, ys, xs = lax.axis_size("rows"), lax.axis_size("cx"), lax.axis_size("cy") // CORES
    chips = ys * xs
    shards = chips * CORES
    batch, features = rows_data.shape
    count, width = centroids.shape
    parts = width // LANES
    slots = upper.shape[0]
    half = slots // 2
    block = min(LANES, slots)
    capacity = -(-(2 * batch // shards) // 8) * 8
    spots = shards * capacity
    across = zs * spots // LANES
    joined = across * LANES
    tall = -(-zs // 8) * 8
    padded = -(-across // 8) * 8
    band = min(joined, 512)
    height = min(count, 512)
    na, nb = (ys - 1) * xs, (xs - 1) * ys

    vm = pl.BlockSpec(memory_space=pltpu.VMEM)
    hbm = pl.BlockSpec(memory_space=pl.ANY)
    V = pltpu.VMEM
    dma = lambda n: pltpu.SemaphoreType.DMA((n,))
    scratch = dict(
        oc=V((1, count), i32), sc=V((count // LANES, LANES), i32), cent=V((count, width), f32),
        owner=V((1, batch), i32), slot=V((1, batch), i32), rows=V((batch, features), f32),
        counts=V((count // LANES, LANES), f32), upper=V((slots, width), f32),
        weights=V((slots // block, block), f32),
        own=V((count // LANES, LANES), i32), uid=V((count // LANES, LANES), f32),
        cp=V((parts, count, 2 * LANES), bf16), oh=V((2, slots, count), bf16),
        outp=V((parts * chips, slots, LANES), f32), pair=V((parts * chips, slots, LANES), f32),
        base=V((parts * chips, slots, LANES), f32), chip=V((parts * chips, slots, LANES), f32),
        info=V((8, LANES), i32), mine=V((zs, 8, LANES), i32),
        slabs=V((parts * zs, batch, LANES), f32), pick=V((zs, spots, LANES), bf16),
        packed=V((parts * zs, spots, LANES), f32), inbox=V((parts, joined, LANES), f32),
        tags=V((tall, spots), i32), heard=V((shards, tall, spots), i32),
        ha=V((shards * 8, count), bf16), hb=V((LANES, count), bf16), hist=V((shards * 8, LANES), f32),
        hs=V((shards, 8, LANES), f32), lab=V((padded, LANES), f32), urow=V((padded, LANES), f32),
        prow=V((padded, LANES), f32), ot=V((band, count), bf16), tab=V((LANES, 5 * LANES), bf16), share=V((joined, LANES), f32),
        near=V((parts, joined, LANES), f32), dl=V((parts, joined, LANES), f32),
        pd=V((parts, joined, LANES), f32), dd=V((parts, 2 * joined, 2 * LANES), bf16),
        oh3=V((chips if parts > 1 else 1, slots, 2 * joined), bf16),
        a1=V((parts * na, half, LANES), f32), b1=V((parts * nb, half, LANES), f32),
        a2=V((parts * (xs - 1), half, LANES), f32), b2=V((parts * (ys - 1), half, LANES), f32),
        relay_a=V((parts * (xs - 1), half, LANES), f32), relay_b=V((parts * (ys - 1), half, LANES), f32),
        dp=V((joined, (2 * parts + 1) * LANES), bf16), oh1=V((height, joined), bf16),
        sums=V((height, (2 * parts + 1) * LANES), f32), fin=V((slots, LANES), f32), mcol=V((slots, LANES), f32), ncol=V((slots, LANES), f32),
        ld=dma(9), si=dma(zs - 1), ri=dma(zs - 1), ss=dma(parts * (zs - 1)), rs=dma(parts * (zs - 1)),
        sp=dma((shards - 1) * zs * parts), rp=dma((shards - 1) * zs * parts),
        st=dma(shards - 1), rt=dma(shards - 1), sh=dma(shards - 1), rh=dma(shards - 1),
        sb=dma(parts * chips), rb=dma(parts * chips), su=dma(1), ru=dma(1), sd=dma(parts), rd=dma(parts),
        sa1=dma(parts * na), ra1=dma(parts * na), sb1=dma(parts * nb), rb1=dma(parts * nb),
        sa2=dma(parts * (xs - 1)), ra2=dma(parts * (xs - 1)), sb2=dma(parts * (ys - 1)), rb2=dma(parts * (ys - 1)),
    )
    outs = (
        jax.ShapeDtypeStruct((count, width), f32),
        jax.ShapeDtypeStruct((count // LANES, LANES), f32),
        jax.ShapeDtypeStruct((slots, width), f32),
        jax.ShapeDtypeStruct((slots // block, block), f32),
    )
    made = pl.pallas_call(
        functools.partial(fused_kernel, tuple(scratch), (zs, ys, xs, capacity, height)),
        out_shape=outs,
        in_specs=[pl.BlockSpec(memory_space=pltpu.HBM)] * 9,
        out_specs=(vm,) * 4,
        scratch_shapes=list(scratch.values()),
        compiler_params=pltpu.CompilerParams(
            collective_id=1, has_side_effects=True, vmem_limit_bytes=44 * 1024 * 1024
        ),
        name="update",
    )(*[pltpu.with_memory_space_constraint(a, pltpu.HBM) for a in (
        rows_data, owner_rows.reshape(1, batch), slot_rows.reshape(1, batch), centroids,
        counts.reshape(-1, LANES), owner_cent.reshape(1, count), slot_cent.reshape(-1, LANES),
        upper, upper_counts.reshape(-1, block),
    )])
    moved, news, new_upper, upnews = pl.pallas_call(
        emit_kernel,
        out_shape=outs,
        in_specs=[vm] * 4,
        out_specs=(hbm,) * 4,
        scratch_shapes=[dma(4)],
        compiler_params=pltpu.CompilerParams(vmem_limit_bytes=4 * 1024 * 1024),
        name="emit",
    )(*made)
    return moved, news.reshape(-1), new_upper, upnews.reshape(-1)


def solution(mesh):
    placed = (
        P(("rows", "cx", "cy"), None),
        P(("rows", "cx", "cy"), None),
        P(("rows", "cx", "cy")),
        P(("cx", "cy"), "rows"),
        P(("cx", "cy")),
        P(("cx", "cy"), None),
        P(("cx", "cy")),
        P(("cx", "cy"), "rows"),
        P(("cx", "cy")),
    )
    return jax.shard_map(
        body,
        mesh=mesh,
        in_specs=placed,
        out_specs=(
            P(("cx", "cy"), "rows"),
            P(("cx", "cy")),
            P(("cx", "cy"), "rows"),
            P(("cx", "cy")),
        ),
        check_vma=False,
    )
```
